128 devices in a mesh: dp: 1, cpo: 16 (over z, y), cpi: 8 (over x, core).
Axes of the slice: x: 4, y: 4, z: 4, core: 2. Of those that a mesh axis runs over, the one named last changes fastest.
Arguments:
- hidden: bfloat16 [16384, 2048], P(('dp', 'cpo', 'cpi'))
- w_q: bfloat16 [2048, 16, 128], replicated
- w_k: bfloat16 [2048, 2, 128], replicated
- w_v: bfloat16 [2048, 2, 128], replicated
- w_o: bfloat16 [16, 128, 2048], replicated
Outputs:
- output: bfloat16 [16384, 2048], P(('dp', 'cpo', 'cpi'))
All inputs are finite; a program needn't handle non-finite values.
Results may differ from the reference program's by a relative error of at most 0.00605925.
Values are sent between devices in bfloat16 or wider.
A program may use at most 1 GiB of HBM per device.

```python
import jax
import jax.numpy as jnp
from jax import lax

D_MODEL = 2048
HEADS_Q = 16
HEADS_KV = 2
HEAD_DIM = 128
TOK_DEV = 128
CHUNKS = 128
WINDOW = 2048
QUERY_BLOCK = 128
SEQ_LEN = CHUNKS * TOK_DEV
GROUP_SIZE = HEADS_Q // HEADS_KV
KEY_SPAN = WINDOW + QUERY_BLOCK
ROPE_BASE = 10000.0


def setup_inputs(seed: int = 0, part: int = 0) -> dict:
    root_part, root_shared = jax.random.split(jax.random.key(seed))
    key_noise, key_shift = jax.random.split(jax.random.fold_in(root_part, part))
    key_q, key_k, key_v, key_o = jax.random.split(root_shared, 4)
    noise = jax.random.normal(key_noise, (CHUNKS, TOK_DEV, D_MODEL), jnp.float32)
    shifts = jax.random.normal(key_shift, (CHUNKS, 1, D_MODEL), jnp.float32)
    hidden = (0.8 * noise + 0.8 * shifts).reshape(SEQ_LEN, D_MODEL).astype(jnp.bfloat16)
    scale_in = D_MODEL ** -0.5
    scale_out = (HEADS_Q * HEAD_DIM) ** -0.5
    w_q = (jax.random.normal(key_q, (D_MODEL, HEADS_Q, HEAD_DIM), jnp.float32) * scale_in).astype(jnp.bfloat16)
    w_k = (jax.random.normal(key_k, (D_MODEL, HEADS_KV, HEAD_DIM), jnp.float32) * scale_in).astype(jnp.bfloat16)
    w_v = (jax.random.normal(key_v, (D_MODEL, HEADS_KV, HEAD_DIM), jnp.float32) * scale_in).astype(jnp.bfloat16)
    w_o = (jax.random.normal(key_o, (HEADS_Q, HEAD_DIM, D_MODEL), jnp.float32) * scale_out).astype(jnp.bfloat16)
    return {'hidden': hidden, 'w_q': w_q, 'w_k': w_k, 'w_v': w_v, 'w_o': w_o}


def rope_rotate(vals, positions):
    half_dim = HEAD_DIM // 2
    inv_freq = ROPE_BASE ** (-jnp.arange(half_dim, dtype=jnp.float32) * 2.0 / HEAD_DIM)
    angles = positions.astype(jnp.float32)[..., None] * inv_freq
    cos_t = jnp.cos(angles)[..., None, :]
    sin_t = jnp.sin(angles)[..., None, :]
    lower_half = vals[..., :half_dim]
    upper_half = vals[..., half_dim:]
    return jnp.concatenate([lower_half * cos_t - upper_half * sin_t, upper_half * cos_t + lower_half * sin_t], axis=-1)


def reference(hidden, w_q, w_k, w_v, w_o):
    positions = jnp.arange(SEQ_LEN)
    q_proj = jnp.dot(hidden, w_q.reshape(D_MODEL, HEADS_Q * HEAD_DIM), preferred_element_type=jnp.float32)
    k_proj = jnp.dot(hidden, w_k.reshape(D_MODEL, HEADS_KV * HEAD_DIM), preferred_element_type=jnp.float32)
    v_proj = jnp.dot(hidden, w_v.reshape(D_MODEL, HEADS_KV * HEAD_DIM), preferred_element_type=jnp.float32)
    q_rot = rope_rotate(q_proj.reshape(SEQ_LEN, HEADS_Q, HEAD_DIM), positions).astype(jnp.bfloat16)
    k_rot = rope_rotate(k_proj.reshape(SEQ_LEN, HEADS_KV, HEAD_DIM), positions).astype(jnp.bfloat16)
    v_val = v_proj.reshape(SEQ_LEN, HEADS_KV, HEAD_DIM).astype(jnp.bfloat16)
    k_pad = jnp.concatenate([jnp.zeros((WINDOW, HEADS_KV, HEAD_DIM), jnp.bfloat16), k_rot], axis=0)
    v_pad = jnp.concatenate([jnp.zeros((WINDOW, HEADS_KV, HEAD_DIM), jnp.bfloat16), v_val], axis=0)
    score_scale = HEAD_DIM ** -0.5
    q_offsets = jnp.arange(QUERY_BLOCK)
    k_offsets = jnp.arange(KEY_SPAN)

    def attend_block(block_idx):
        q_start = block_idx * QUERY_BLOCK
        q_blk = lax.dynamic_slice_in_dim(q_rot, q_start, QUERY_BLOCK, 0).reshape(QUERY_BLOCK, HEADS_KV, GROUP_SIZE, HEAD_DIM)
        k_blk = lax.dynamic_slice_in_dim(k_pad, q_start, KEY_SPAN, 0)
        v_blk = lax.dynamic_slice_in_dim(v_pad, q_start, KEY_SPAN, 0)
        scores = jnp.einsum('tkgd,skd->kgts', q_blk.astype(jnp.float32), k_blk.astype(jnp.float32)) * score_scale
        pos_gap = q_offsets[:, None] + WINDOW - k_offsets[None, :]
        key_pos = q_start - WINDOW + k_offsets
        allowed = (pos_gap >= 0) & (pos_gap < WINDOW) & (key_pos[None, :] >= 0)
        scores = jnp.where(allowed, scores, -jnp.inf)
        row_max = jnp.max(scores, axis=-1, keepdims=True)
        exp_scores = jnp.exp(scores - row_max)
        exp_total = jnp.sum(exp_scores, axis=-1)
        weighted = jnp.einsum('kgts,skd->kgtd', exp_scores.astype(jnp.bfloat16).astype(jnp.float32), v_blk.astype(jnp.float32))
        return (weighted / exp_total[..., None]).astype(jnp.bfloat16)

    attended = lax.map(attend_block, jnp.arange(SEQ_LEN // QUERY_BLOCK))
    attended = jnp.transpose(attended, (0, 3, 1, 2, 4)).reshape(SEQ_LEN, HEADS_Q * HEAD_DIM)
    out_proj = jnp.dot(attended, w_o.reshape(HEADS_Q * HEAD_DIM, D_MODEL), preferred_element_type=jnp.float32)
    return out_proj.astype(jnp.bfloat16)
```

```python
import functools
import math

import jax
import jax.numpy as jnp
import numpy as np
from jax import lax
from jax.experimental import pallas as pl
from jax.experimental.pallas import tpu as pltpu
from jax.sharding import PartitionSpec as P

WINDOW = 2048
ROPE_BASE = 10000.0
MESH = pl.DeviceIdType.MESH
F32, BF16 = jnp.float32, jnp.bfloat16
NEG = -jnp.inf


def rope_tables(tok_chip, n_chips, head_dim):
    half = head_dim // 2
    freq = ROPE_BASE ** (-np.arange(half, dtype=np.float64) * 2.0 / head_dim)
    local = np.arange(tok_chip, dtype=np.float64)[:, None] * freq
    base = (np.arange(n_chips, dtype=np.float64) * tok_chip)[:, None] * freq
    dup = lambda a: np.concatenate([a, a], axis=-1)
    loc = np.stack([dup(np.cos(local)), dup(np.sin(local))]).astype(np.float32)
    bas = np.stack([dup(np.cos(base)), dup(np.sin(base))]).astype(np.float32)
    return loc, bas


def kernel(dims, x_hbm, wq_hbm, wk_hbm, wv_hbm, wo_hbm, loc_hbm, bas_hbm, y_hbm,
           x2, wqr, wkr, wvr, wqb, wkvb, wob, loc, bas, f32a, f32b, own, kv, q_t, cs_t, m_s, l_s, acc, o_all, o_send, y_v, y_b,
           ld_sem, wq_sem, y_sem, xs_sem, xr_sem, ps_sem, pr_sem, ks_sem, kr_sem, os_sem, or_sem):
    n_outer, n_inner, tok, dm, g, hd, nb = dims
    n_chips = n_outer * n_inner // 2
    rank = lax.axis_index("cpo") * n_inner + lax.axis_index("cpi")
    c = lax.div(rank, 2)
    h = lax.rem(rank, 2)
    oh = 1 - h

    def dev(chip, core):
        r = chip * 2 + core
        return {"cpo": lax.div(r, n_inner), "cpi": lax.rem(r, n_inner)}

    def load(src, dst, sem):
        cp = pltpu.make_async_copy(src, dst, sem)
        cp.start()
        return cp

    barrier = pltpu.get_barrier_semaphore()
    pl.semaphore_signal(barrier, inc=1, device_id=dev(c, oh), device_id_type=MESH)
    for j in range(1, nb):
        @pl.when(c - j >= 0)
        def _():
            for hh in range(2):
                pl.semaphore_signal(barrier, inc=1, device_id=dev(c - j, hh), device_id_type=MESH)

    ld_x = load(x_hbm, x2.at[h], ld_sem.at[0])
    ld_k = load(wk_hbm, wkr, ld_sem.at[1])
    ld_v = load(wv_hbm, wvr, ld_sem.at[2])
    ld_l = load(loc_hbm, loc, ld_sem.at[3])
    ld_b = load(bas_hbm, bas, ld_sem.at[4])
    n_wq = wq_sem.shape[0]
    rows_wq = dm // n_wq
    head0 = pl.multiple_of(h * g, g)
    ld_q = [load(wq_hbm.at[pl.ds(i * rows_wq, rows_wq), pl.ds(head0, g), :], wqr.at[pl.ds(i * rows_wq, rows_wq)], wq_sem.at[i])
            for i in range(n_wq)]

    chunk = f32a.shape[0]
    for raw, ld, col in ((wkr, ld_k, 0), (wvr, ld_v, 1)):
        ld.wait()

        def relay_kv(i, _):
            r0 = pl.multiple_of(i * 2 * chunk, 2 * chunk)
            d0 = pl.multiple_of(i * chunk, chunk)
            for part, buf in enumerate((f32a, f32b)):
                buf[...] = raw[pl.ds(r0 + part * chunk, chunk), :].astype(F32)
                for hh in range(2):
                    piece = buf[pl.ds(hh, chunk // 2, stride=2), :].astype(BF16)
                    wkvb[pl.ds(d0 + part * (chunk // 2), chunk // 2), pl.ds((2 * hh + col) * hd, hd)] = piece
            return 0

        lax.fori_loop(0, 2 * dm // (2 * chunk), relay_kv, 0)

    ld_x.wait()
    n_tgt = jnp.minimum(nb - 1, n_chips - 1 - c)
    pl.semaphore_wait(barrier, 1 + 2 * n_tgt)
    x_copy = pltpu.make_async_remote_copy(src_ref=x2.at[h], dst_ref=x2.at[h], send_sem=xs_sem, recv_sem=xr_sem,
                                          device_id=dev(c, oh), device_id_type=MESH)
    x_copy.start()
    kvp = jnp.dot(x2[h], wkvb[...], preferred_element_type=F32)
    ld_l.wait()
    ld_b.wait()
    t0 = pl.multiple_of(h * tok, tok)
    cb, sb = bas[0, pl.ds(c, 1), :], bas[1, pl.ds(c, 1), :]
    cl, sl = loc[0, pl.ds(t0, tok), :], loc[1, pl.ds(t0, tok), :]
    cos_k = cl * cb - sl * sb
    sin_k = sl * cb + cl * sb
    lane = lax.broadcasted_iota(jnp.int32, (tok, hd), 1)
    sin_k = jnp.where(lane < hd // 2, -sin_k, sin_k)
    for hh in range(2):
        k = kvp[:, 2 * hh * hd:(2 * hh + 1) * hd]
        k = (k * cos_k + pltpu.roll(k, hd // 2, 1) * sin_k).astype(BF16)
        v = kvp[:, (2 * hh + 1) * hd:(2 * hh + 2) * hd]
        own[hh, 0] = k
        own[hh, 1] = v.T.astype(BF16)
    kv[0, h] = own[h]

    p_copy = pltpu.make_async_remote_copy(src_ref=own.at[oh], dst_ref=kv.at[0, h], send_sem=ps_sem, recv_sem=pr_sem,
                                          device_id=dev(c, oh), device_id_type=MESH)
    p_copy.start()

    def kv_copy(j, hh, chip):
        return pltpu.make_async_remote_copy(src_ref=own.at[hh], dst_ref=kv.at[j, h], send_sem=ks_sem.at[j, hh], recv_sem=kr_sem.at[j, h],
                                            device_id=dev(chip, hh), device_id_type=MESH)

    for j in range(1, nb):
        @pl.when(c + j < n_chips)
        def _():
            for hh in range(2):
                kv_copy(j, hh, c + j).start()

    ld_o = load(wo_hbm, wob, ld_sem.at[5])

    dch = chunk // g
    for i in range(n_wq):
        ld_q[i].wait()

        def relay_q(t, _):
            d0 = pl.multiple_of(i * rows_wq + t * 2 * dch, 2 * dch)
            for part, buf in enumerate((f32a, f32b)):
                dd = pl.multiple_of(d0 + part * dch, dch)
                buf[...] = wqr[pl.ds(dd, dch)].astype(F32).reshape(chunk, hd)
                for n in range(g):
                    wqb[pl.ds(dd, dch), n * hd:(n + 1) * hd] = buf[pl.ds(n, dch, stride=g), :].astype(BF16)
            return 0

        lax.fori_loop(0, rows_wq // (2 * dch), relay_q, 0)
    half = hd // 2
    cl, sl = loc[0], loc[1]
    cs_t[0] = (cl * cb - sl * sb).T[:half]
    cs_t[1] = (sl * cb + cl * sb).T[:half]
    x_copy.wait_recv()
    xall = x2[...].reshape(2 * tok, dm)

    def proj_q(n, _):
        c0 = pl.multiple_of(n * 2 * hd, 2 * hd)
        qp = jnp.dot(xall, wqb[:, pl.ds(c0, 2 * hd)], preferred_element_type=F32)
        for s in range(2):
            qt = qp[:, s * hd:(s + 1) * hd].T
            lo, hi = qt[:half], qt[half:]
            q_t[2 * n + s, :half] = (lo * cs_t[0] - hi * cs_t[1]).astype(BF16)
            q_t[2 * n + s, half:] = (hi * cs_t[0] + lo * cs_t[1]).astype(BF16)
        return 0

    lax.fori_loop(0, g // 2, proj_q, 0)

    scale = hd ** -0.5 * math.log2(math.e)
    ki = lax.broadcasted_iota(jnp.int32, (2 * tok, 2 * tok), 0)
    qi = lax.broadcasted_iota(jnp.int32, (2 * tok, 2 * tok), 1)

    def attend(j):
        def head(n, _):
            kb = kv[j, :, 0].reshape(2 * tok, hd)
            vb = jnp.concatenate([kv[j, 0, 1], kv[j, 1, 1]], axis=1)
            s = jnp.dot(kb, q_t[n], preferred_element_type=F32) * scale
            if j == 0:
                s = jnp.where(ki <= qi, s, NEG)
            if j == nb - 1:
                s = jnp.where(ki > qi, s, NEG)
            top = jnp.max(s, axis=0, keepdims=True)
            if j == 0:
                m_new = top
                p = jnp.exp2(s - m_new)
                l_s[n] = jnp.sum(p, axis=0, keepdims=True)
                acc[n] = jnp.dot(vb, p.astype(BF16), preferred_element_type=F32)
            else:
                m_old = m_s[n]
                m_new = jnp.maximum(m_old, top)
                p = jnp.exp2(s - m_new)
                alpha = jnp.exp2(m_old - m_new)
                l_s[n] = l_s[n] * alpha + jnp.sum(p, axis=0, keepdims=True)
                acc[n] = acc[n] * alpha + jnp.dot(vb, p.astype(BF16), preferred_element_type=F32)
            m_s[n] = m_new
            return 0

        lax.fori_loop(0, g, head, 0)

    p_copy.wait_recv()
    attend(0)
    for j in range(1, nb):
        @pl.when(c - j >= 0)
        def _():
            for s in range(2):
                pltpu.make_async_copy(own.at[0], kv.at[j, s], kr_sem.at[j, s]).wait()
            attend(j)

    def finish(n, _):
        o = (acc[n] / l_s[n]).T.astype(BF16)
        c0 = pl.multiple_of(n * hd, hd)
        o_send[0, :, pl.ds(c0, hd)] = o[:tok]
        o_send[1, :, pl.ds(c0, hd)] = o[tok:]
        return 0

    lax.fori_loop(0, g, finish, 0)
    o_copy = pltpu.make_async_remote_copy(src_ref=o_send.at[oh], dst_ref=o_all, send_sem=os_sem, recv_sem=or_sem,
                                          device_id=dev(c, oh), device_id_type=MESH)
    o_copy.start()
    ld_o.wait()
    w0 = pl.multiple_of(h * g * hd, g * hd)
    w1 = pl.multiple_of(oh * g * hd, g * hd)
    o_own = o_send[h]
    n_y = y_sem.shape[0]
    cols = dm // n_y

    def own_part(i, _):
        c0 = pl.multiple_of(i * cols, cols)
        y_v[:, pl.ds(c0, cols)] = jnp.dot(o_own, wob[pl.ds(w0, g * hd), pl.ds(c0, cols)], preferred_element_type=F32)
        return 0

    lax.fori_loop(0, n_y, own_part, 0)
    o_copy.wait_recv()
    o_oth = o_all[...]
    outs = []
    for i in range(n_y):
        cs = slice(i * cols, (i + 1) * cols)
        y_b[:, cs] = (y_v[:, cs] + jnp.dot(o_oth, wob[pl.ds(w1, g * hd), cs], preferred_element_type=F32)).astype(BF16)
        outs.append(load(y_b.at[:, cs], y_hbm.at[:, cs], y_sem.at[i]))
    for cp in outs:
        cp.wait()
    x_copy.wait_send()
    p_copy.wait_send()
    o_copy.wait_send()
    for j in range(1, nb):
        @pl.when(c + j < n_chips)
        def _():
            for hh in range(2):
                kv_copy(j, hh, c + j).wait_send()


def solution(mesh):
    n_outer, n_inner = mesh.shape['cpo'], mesh.shape['cpi']

    def local_fn(hidden, w_q, w_k, w_v, w_o):
        tok, dm = hidden.shape
        hq, hd = w_q.shape[1], w_q.shape[2]
        g = hq // 2
        nb = WINDOW // (2 * tok) + 1
        loc, bas = rope_tables(2 * tok, n_outer * n_inner // 2, hd)
        dims = (n_outer, n_inner, tok, dm, g, hd, nb)
        chunk = 1024
        scratch = [
            pltpu.VMEM((2, tok, dm), BF16), pltpu.VMEM((dm, g, hd), BF16), pltpu.VMEM((2 * dm, hd), BF16), pltpu.VMEM((2 * dm, hd), BF16),
            pltpu.VMEM((dm, g * hd), BF16), pltpu.VMEM((dm, 4 * hd), BF16), pltpu.VMEM((hq * hd, dm), BF16),
            pltpu.VMEM(loc.shape, F32), pltpu.VMEM(bas.shape, F32),
            pltpu.VMEM((chunk, hd), F32), pltpu.VMEM((chunk, hd), F32),
            pltpu.VMEM((2, 2, tok, hd), BF16), pltpu.VMEM((nb, 2, 2, tok, hd), BF16),
            pltpu.VMEM((g, hd, 2 * tok), BF16), pltpu.VMEM((2, hd // 2, 2 * tok), F32),
            pltpu.VMEM((g, 1, 2 * tok), F32), pltpu.VMEM((g, 1, 2 * tok), F32), pltpu.VMEM((g, hd, 2 * tok), F32),
            pltpu.VMEM((tok, g * hd), BF16), pltpu.VMEM((2, tok, g * hd), BF16), pltpu.VMEM((tok, dm), F32), pltpu.VMEM((tok, dm), BF16),
            pltpu.SemaphoreType.DMA((6,)), pltpu.SemaphoreType.DMA((4,)), pltpu.SemaphoreType.DMA((4,)),
            pltpu.SemaphoreType.DMA, pltpu.SemaphoreType.DMA, pltpu.SemaphoreType.DMA, pltpu.SemaphoreType.DMA,
            pltpu.SemaphoreType.DMA((nb, 2)), pltpu.SemaphoreType.DMA((nb, 2)), pltpu.SemaphoreType.DMA, pltpu.SemaphoreType.DMA,
        ]
        return pl.pallas_call(
            functools.partial(kernel, dims),
            out_shape=jax.ShapeDtypeStruct((tok, dm), BF16),
            in_specs=[pl.BlockSpec(memory_space=pl.ANY)] * 7,
            out_specs=pl.BlockSpec(memory_space=pl.ANY),
            scratch_shapes=scratch,
            compiler_params=pltpu.CompilerParams(collective_id=0, has_side_effects=True, vmem_limit_bytes=56 * 1024 * 1024),
        )(hidden, w_q, w_k.reshape(2 * dm, hd), w_v.reshape(2 * dm, hd), w_o.reshape(hq * hd, dm), jnp.asarray(loc), jnp.asarray(bas))

    return jax.shard_map(local_fn, mesh=mesh,
                         in_specs=(P(('dp', 'cpo', 'cpi'), None), P(), P(), P(), P()),
                         out_specs=P(('dp', 'cpo', 'cpi'), None), check_vma=False)
```

```python
import functools
import math

import jax
import jax.numpy as jnp
import numpy as np
from jax import lax
from jax.experimental import pallas as pl
from jax.experimental.pallas import tpu as pltpu
from jax.sharding import PartitionSpec as P

WINDOW = 2048
ROPE_BASE = 10000.0
MESH = pl.DeviceIdType.MESH
F32, BF16 = jnp.float32, jnp.bfloat16


def rope_tables(tok_chip, n_chips, head_dim):
    half = head_dim // 2
    freq = ROPE_BASE ** (-np.arange(half, dtype=np.float64) * 2.0 / head_dim)
    local = np.arange(tok_chip, dtype=np.float64)[:, None] * freq
    base = (np.arange(n_chips, dtype=np.float64) * tok_chip)[:, None] * freq
    dup = lambda a: np.concatenate([a, a], axis=-1)
    loc = np.stack([dup(np.cos(local)), dup(np.sin(local))]).astype(np.float32)
    bas = np.stack([dup(np.cos(base)), dup(np.sin(base))]).astype(np.float32)
    return loc, bas


def kernel(dims, x_hbm, wq_hbm, wk_hbm, wv_hbm, wo_hbm, loc_hbm, bas_hbm, y_hbm,
           x2, wqr, wkr, wvr, wqb, wkvb, wob, loc, bas, f32a, f32b, own, kv, q_t, cs_t, m_s, l_s, acc, o_all, o_send, y_v, y_b,
           ld_sem, wq_sem, y_sem, xs_sem, xr_sem, ps_sem, pr_sem, ks_sem, kr_sem, rs_sem, rr_sem, os_sem, or_sem):
    n_outer, n_inner, tok, dm, g, hd, nb = dims
    n_row = n_inner // 2
    n_chips = n_outer * n_inner // 2
    rank = lax.axis_index("cpo") * n_inner + lax.axis_index("cpi")
    c = lax.div(rank, 2)
    h = lax.rem(rank, 2)
    oh = 1 - h

    def dev(chip, core):
        r = chip * 2 + core
        return {"cpo": lax.div(r, n_inner), "cpi": lax.rem(r, n_inner)}

    def load(src, dst, sem):
        cp = pltpu.make_async_copy(src, dst, sem)
        cp.start()
        return cp

    row, col = lax.div(c, n_row), lax.rem(c, n_row)
    n_rows = n_chips // n_row
    last = nb - 1


    barrier = pltpu.get_barrier_semaphore()

    def greet(chip, core):
        pl.semaphore_signal(barrier, inc=1, device_id=dev(chip, core), device_id_type=MESH)

    right = row * n_row + lax.rem(col + 1, n_row)
    left = row * n_row + lax.rem(col + n_row - 1, n_row)
    one = lambda cond: jnp.where(cond, 1, 0)
    both = jnp.logical_and
    up1, up2, dn1, dn2 = row + 1 < n_rows, row + 2 < n_rows, row >= 1, row >= 2

    odd = lax.rem(row, 2) == 1
    direct = [(up1, 4, c + 4), (col < 3, 1, c + 1), (col < 1, 3, c + 3), (col < 2, 2, c + 2), (both(up2, odd), 8, c + 8)]
    later = [(both(up2, jnp.logical_not(odd)), 8, c + 8), (both(up1, col == 3), 5, c + 1)]
    origin = [(dn1, c - 4), (col >= 1, c - 1), (both(dn1, col == 0), c - 1), (dn2, c - 8), (col >= 3, c - 3), (col >= 2, c - 2)]
    relay_row = [(both(dn1, col < 3), 4, 5, right), (dn1, 4, 7, left)]
    relay_far = [(both(dn2, col >= 1), 8, 3, left), (both(dn2, col == 3), 8, 1, right), (both(dn2, col >= 2), 8, 2, c - 2)]
    relay_5 = [(both(dn1, col < 2), 5, 6, right)]
    relay_7 = [(both(dn1, col < 2), 7, 6, left)]

    def when_all(cond, act):
        pl.when(cond)(act)

    greet(c, oh)
    for cond, chip in origin:
        when_all(cond, lambda chip=chip: [greet(chip, hh) for hh in range(2)] and None)
    when_all(dn1, lambda: [greet(chip, h) for chip in (left, right)] and None)
    when_all(both(dn2, col < 2), lambda: greet(c + 2, h))
    n_sent = 1 + 2 * one(dn1) + one(both(dn2, col >= 2))
    for cond, _, _ in direct + later:
        n_sent = n_sent + 2 * one(cond)

    ld_x = load(x_hbm, x2.at[h], ld_sem.at[0])
    ld_k = load(wk_hbm, wkr, ld_sem.at[1])
    ld_v = load(wv_hbm, wvr, ld_sem.at[2])
    ld_l = load(loc_hbm, loc, ld_sem.at[3])
    ld_b = load(bas_hbm, bas, ld_sem.at[4])
    chunk = f32a.shape[0]
    with jax.named_scope("relay_kv"):
        for raw, ld, sel in ((wkr, ld_k, 0), (wvr, ld_v, 1)):
            ld.wait()

            def relay_kv(i, _):
                r0 = pl.multiple_of(i * 2 * chunk, 2 * chunk)
                d0 = pl.multiple_of(i * chunk, chunk)
                for part, buf in enumerate((f32a, f32b)):
                    buf[...] = raw[pl.ds(r0 + part * chunk, chunk), :].astype(F32)
                    for hh in range(2):
                        piece = buf[pl.ds(hh, chunk // 2, stride=2), :].astype(BF16)
                        wkvb[pl.ds(d0 + part * (chunk // 2), chunk // 2), pl.ds((2 * hh + sel) * hd, hd)] = piece
                return 0

            lax.fori_loop(0, 2 * dm // (2 * chunk), relay_kv, 0)
    n_wq = wq_sem.shape[0]
    rows_wq = dm // n_wq
    head0 = pl.multiple_of(h * g, g)
    ld_q = [load(wq_hbm.at[pl.ds(i * rows_wq, rows_wq), pl.ds(head0, g), :], wqr.at[pl.ds(i * rows_wq, rows_wq)], wq_sem.at[i])
            for i in range(n_wq)]

    ld_x.wait()
    with jax.named_scope("kvproj"):
        kvp = jnp.dot(x2[h], wkvb[...], preferred_element_type=F32)
    ld_l.wait()
    ld_b.wait()
    t0 = pl.multiple_of(h * tok, tok)
    cb, sb = bas[0, pl.ds(c, 1), :], bas[1, pl.ds(c, 1), :]
    cl, sl = loc[0, pl.ds(t0, tok), :], loc[1, pl.ds(t0, tok), :]
    cos_k = cl * cb - sl * sb
    sin_k = sl * cb + cl * sb
    lane = lax.broadcasted_iota(jnp.int32, (tok, hd), 1)
    sin_k = jnp.where(lane < hd // 2, -sin_k, sin_k)
    for hh in range(2):
        k = kvp[:, 2 * hh * hd:(2 * hh + 1) * hd]
        k = (k * cos_k + pltpu.roll(k, hd // 2, 1) * sin_k).astype(BF16)
        v = kvp[:, (2 * hh + 1) * hd:(2 * hh + 2) * hd]
        own[hh, 0] = k
        own[hh, 1] = v.T.astype(BF16)
    kv[0, h] = own[h]

    with jax.named_scope("barrier"):
        pl.semaphore_wait(barrier, n_sent)
    x_copy = pltpu.make_async_remote_copy(src_ref=x2.at[h], dst_ref=x2.at[h], send_sem=xs_sem, recv_sem=xr_sem,
                                          device_id=dev(c, oh), device_id_type=MESH)

    p_copy = pltpu.make_async_remote_copy(src_ref=own.at[oh], dst_ref=kv.at[0, h], send_sem=ps_sem, recv_sem=pr_sem,
                                          device_id=dev(c, oh), device_id_type=MESH)
    p_copy.start()

    def each_direct(act, first, group):
        for i, (cond, slot, chip) in enumerate(group, first):
            @pl.when(cond)
            def _():
                for hh in range(2):
                    act(pltpu.make_async_remote_copy(src_ref=own.at[hh], dst_ref=kv.at[slot, h], send_sem=ks_sem.at[i, hh],
                                                     recv_sem=kr_sem.at[slot, h], device_id=dev(chip, hh), device_id_type=MESH))

    relays = relay_row + relay_far + relay_5 + relay_7

    def each_relay(act, group):
        for item in group:
            cond, src, dst, chip = item
            i = [r is item for r in relays].index(True)

            @pl.when(cond)
            def _():
                act(pltpu.make_async_remote_copy(src_ref=kv.at[src], dst_ref=kv.at[dst], send_sem=rs_sem.at[i], recv_sem=rr_sem.at[dst],
                                                 device_id=dev(chip, h), device_id_type=MESH))

    each_direct(lambda cp: cp.start(), 0, direct)
    x_copy.start()

    ld_o = load(wo_hbm, wob, ld_sem.at[5])

    with jax.named_scope("relay_q"):
        dch = chunk // g
        for i in range(n_wq):
            ld_q[i].wait()

            def relay_q(t, _):
                d0 = pl.multiple_of(i * rows_wq + t * 2 * dch, 2 * dch)
                for part, buf in enumerate((f32a, f32b)):
                    dd = pl.multiple_of(d0 + part * dch, dch)
                    buf[...] = wqr[pl.ds(dd, dch)].astype(F32).reshape(chunk, hd)
                    for n in range(g):
                        wqb[pl.ds(dd, dch), n * hd:(n + 1) * hd] = buf[pl.ds(n, dch, stride=g), :].astype(BF16)
                return 0

            lax.fori_loop(0, rows_wq // (2 * dch), relay_q, 0)
    each_direct(lambda cp: cp.start(), len(direct), later)
    half = hd // 2
    cl, sl = loc[0], loc[1]
    cs_t[0] = (cl * cb - sl * sb).T[:half]
    cs_t[1] = (sl * cb + cl * sb).T[:half]
    with jax.named_scope("xwait"):
        x_copy.wait_recv()
    xall = x2[...].reshape(2 * tok, dm)

    def proj_q(n, _):
        c0 = pl.multiple_of(n * 2 * hd, 2 * hd)
        qp = jnp.dot(xall, wqb[:, pl.ds(c0, 2 * hd)], preferred_element_type=F32)
        for s in range(2):
            qt = qp[:, s * hd:(s + 1) * hd].T
            lo, hi = qt[:half], qt[half:]
            q_t[2 * n + s, :half] = (lo * cs_t[0] - hi * cs_t[1]).astype(BF16)
            q_t[2 * n + s, half:] = (hi * cs_t[0] + lo * cs_t[1]).astype(BF16)
        return 0

    with jax.named_scope("qproj"):
        lax.fori_loop(0, g // 2, proj_q, 0)
    scale = hd ** -0.5 * math.log2(math.e)
    ki = lax.broadcasted_iota(jnp.int32, (2 * tok, 2 * tok), 0)
    qi = lax.broadcasted_iota(jnp.int32, (2 * tok, 2 * tok), 1)

    def attend(slot):
        kb = kv[slot, :, 0].reshape(2 * tok, hd)
        vb = jnp.concatenate([kv[slot, 0, 1], kv[slot, 1, 1]], axis=1)

        def weigh(n, s):
            if slot == 0:
                s = jnp.where(ki <= qi, s, -jnp.inf)
            if slot == last:
                s = jnp.where(ki > qi, s, -jnp.inf)
            top = jnp.max(s, axis=0, keepdims=True) * scale
            m_new = top if slot == 0 else jnp.maximum(m_s[n], top)
            p = jnp.exp2(s * scale - m_new)
            tot = jnp.sum(p, axis=0, keepdims=True)
            alpha = None
            if slot == 0:
                l_s[n] = tot
            else:
                alpha = jnp.exp2(m_s[n] - m_new)
                l_s[n] = l_s[n] * alpha + tot
            m_s[n] = m_new
            return p.astype(BF16), alpha

        def gather(n, p, alpha):
            r = jnp.dot(vb, p, preferred_element_type=F32)
            acc[n] = r if alpha is None else acc[n] * alpha + r

        scores, held = [], None
        for n in range(g):
            while len(scores) < min(n + 3, g):
                scores.append(jnp.dot(kb, q_t[len(scores)], preferred_element_type=F32))
            p, alpha = weigh(n, scores[n])
            if held is not None:
                gather(*held)
            held = (n, p, alpha)
        gather(*held)

    def landed(slot, relayed):
        with jax.named_scope(f"w{slot}{'r' * relayed}"):
            if relayed:
                pltpu.make_async_copy(kv.at[0], kv.at[slot], rr_sem.at[slot]).wait()
            else:
                for s in range(2):
                    pltpu.make_async_copy(own.at[0], kv.at[slot, s], kr_sem.at[slot, s]).wait()

    def visit(slot, here, relay=(), got=False, direct_if=None, relayed=False):
        @pl.when(here)
        def _():
            if not got:
                if direct_if is None:
                    landed(slot, relayed)
                else:
                    pl.when(direct_if)(lambda: landed(slot, False))
                    pl.when(jnp.logical_not(direct_if))(lambda: landed(slot, True))
                each_relay(lambda cp: cp.start(), relay)
            with jax.named_scope(f"att{slot}"):
                attend(slot)

    def first_relay(late):
        @pl.when(both(dn1, (lax.rem(row, 4) == 0) == late))
        def _():
            landed(4, False)
            each_relay(lambda cp: cp.start(), relay_row)

    first_relay(False)
    with jax.named_scope("pwait"):
        p_copy.wait_recv()
    with jax.named_scope("att0"):
        attend(0)
    first_relay(True)
    visit(4, dn1, got=True)
    visit(1, col >= 1)
    visit(8, dn2, relay=relay_far)
    visit(2, col >= 2)
    visit(3, col >= 3)
    visit(5, dn1, relay=relay_5, direct_if=col == 0)
    visit(7, dn1, relay=relay_7, relayed=True)
    visit(3, both(dn2, col < 3), relayed=True)
    visit(6, dn1, relayed=True)
    visit(1, both(dn2, col < 1), relayed=True)
    visit(2, both(dn2, col < 2), relayed=True)

    def finish(n, _):
        o = (acc[n] / l_s[n]).T.astype(BF16)
        c0 = pl.multiple_of(n * hd, hd)
        o_send[0, :, pl.ds(c0, hd)] = o[:tok]
        o_send[1, :, pl.ds(c0, hd)] = o[tok:]
        return 0

    with jax.named_scope("finish"):
        lax.fori_loop(0, g, finish, 0, unroll=True)
    o_copy = pltpu.make_async_remote_copy(src_ref=o_send.at[oh], dst_ref=o_all, send_sem=os_sem, recv_sem=or_sem,
                                          device_id=dev(c, oh), device_id_type=MESH)
    o_copy.start()
    with jax.named_scope("wowait"):
        ld_o.wait()
    w0 = pl.multiple_of(h * g * hd, g * hd)
    w1 = pl.multiple_of(oh * g * hd, g * hd)
    o_own = o_send[h]
    n_y = y_sem.shape[0]
    cols = dm // n_y

    def own_part(i, _):
        c0 = pl.multiple_of(i * cols, cols)
        y_v[:, pl.ds(c0, cols)] = jnp.dot(o_own, wob[pl.ds(w0, g * hd), pl.ds(c0, cols)], preferred_element_type=F32)
        return 0

    with jax.named_scope("wo_own"):
        lax.fori_loop(0, n_y, own_part, 0)
    with jax.named_scope("owait"):
        o_copy.wait_recv()
    o_oth = o_all[...]
    outs = []
    with jax.named_scope("wo_oth"):
        for i in range(n_y):
            cs = slice(i * cols, (i + 1) * cols)
            y_b[:, cs] = (y_v[:, cs] + jnp.dot(o_oth, wob[pl.ds(w1, g * hd), cs], preferred_element_type=F32)).astype(BF16)
            outs.append(load(y_b.at[:, cs], y_hbm.at[:, cs], y_sem.at[i]))
    with jax.named_scope("ywait"):
        for cp in outs:
            cp.wait()
    with jax.named_scope("sendwait"):
        x_copy.wait_send()
        p_copy.wait_send()
        o_copy.wait_send()
        each_direct(lambda cp: cp.wait_send(), 0, direct + later)

        each_relay(lambda cp: cp.wait_send(), relays)


def solution(mesh):
    n_outer, n_inner = mesh.shape['cpo'], mesh.shape['cpi']

    def local_fn(hidden, w_q, w_k, w_v, w_o):
        tok, dm = hidden.shape
        hq, hd = w_q.shape[1], w_q.shape[2]
        g = hq // 2
        nb = WINDOW // (2 * tok) + 1
        loc, bas = rope_tables(2 * tok, n_outer * n_inner // 2, hd)
        dims = (n_outer, n_inner, tok, dm, g, hd, nb)
        chunk = 1024
        scratch = [
            pltpu.VMEM((2, tok, dm), BF16), pltpu.VMEM((dm, g, hd), BF16), pltpu.VMEM((2 * dm, hd), BF16), pltpu.VMEM((2 * dm, hd), BF16),
            pltpu.VMEM((dm, g * hd), BF16), pltpu.VMEM((dm, 4 * hd), BF16), pltpu.VMEM((hq * hd, dm), BF16),
            pltpu.VMEM(loc.shape, F32), pltpu.VMEM(bas.shape, F32),
            pltpu.VMEM((chunk, hd), F32), pltpu.VMEM((chunk, hd), F32),
            pltpu.VMEM((2, 2, tok, hd), BF16), pltpu.VMEM((nb, 2, 2, tok, hd), BF16),
            pltpu.VMEM((g, hd, 2 * tok), BF16), pltpu.VMEM((2, hd // 2, 2 * tok), F32),
            pltpu.VMEM((g, 1, 2 * tok), F32), pltpu.VMEM((g, 1, 2 * tok), F32), pltpu.VMEM((g, hd, 2 * tok), F32),
            pltpu.VMEM((tok, g * hd), BF16), pltpu.VMEM((2, tok, g * hd), BF16), pltpu.VMEM((tok, dm), F32), pltpu.VMEM((tok, dm), BF16),
            pltpu.SemaphoreType.DMA((6,)), pltpu.SemaphoreType.DMA((4,)), pltpu.SemaphoreType.DMA((4,)),
            pltpu.SemaphoreType.DMA, pltpu.SemaphoreType.DMA, pltpu.SemaphoreType.DMA, pltpu.SemaphoreType.DMA,
            pltpu.SemaphoreType.DMA((2 * nb, 2)), pltpu.SemaphoreType.DMA((nb, 2)), *[pltpu.SemaphoreType.DMA((nb,))] * 2, pltpu.SemaphoreType.DMA, pltpu.SemaphoreType.DMA,
        ]
        return pl.pallas_call(
            functools.partial(kernel, dims),
            out_shape=jax.ShapeDtypeStruct((tok, dm), BF16),
            in_specs=[pl.BlockSpec(memory_space=pl.ANY)] * 7,
            out_specs=pl.BlockSpec(memory_space=pl.ANY),
            scratch_shapes=scratch,
            compiler_params=pltpu.CompilerParams(collective_id=0, has_side_effects=True, vmem_limit_bytes=56 * 1024 * 1024),
        )(hidden, w_q, w_k.reshape(2 * dm, hd), w_v.reshape(2 * dm, hd), w_o.reshape(hq * hd, dm), jnp.asarray(loc), jnp.asarray(bas))

    return jax.shard_map(local_fn, mesh=mesh,
                         in_specs=(P(('dp', 'cpo', 'cpi'), None), P(), P(), P(), P()),
                         out_specs=P(('dp', 'cpo', 'cpi'), None), check_vma=False)
```

```python
import functools
import math

import jax
import jax.numpy as jnp
import numpy as np
from jax import lax
from jax.experimental import pallas as pl
from jax.experimental.pallas import tpu as pltpu
from jax.sharding import PartitionSpec as P

WINDOW = 2048
ROPE_BASE = 10000.0
MESH = pl.DeviceIdType.MESH
F32, BF16 = jnp.float32, jnp.bfloat16


def rope_tables(tok_chip, n_chips, head_dim):
    half = head_dim // 2
    freq = ROPE_BASE ** (-np.arange(half, dtype=np.float64) * 2.0 / head_dim)
    local = np.arange(tok_chip, dtype=np.float64)[:, None] * freq
    base = (np.arange(n_chips, dtype=np.float64) * tok_chip)[:, None] * freq
    dup = lambda a: np.concatenate([a, a], axis=-1)
    loc = np.stack([dup(np.cos(local)), dup(np.sin(local))]).astype(np.float32)
    bas = np.stack([dup(np.cos(base)), dup(np.sin(base))]).astype(np.float32)
    return loc, bas


def kernel(dims, x_hbm, wq_hbm, wk_hbm, wv_hbm, wo_hbm, loc_hbm, bas_hbm, y_ref,
           x2, wqr, wkr, wvr, big, wob, loc, bas, own, kv, q_t, cs_t, m_s, l_s, acc, o_all, o_send, y_v,
           ld_sem, wq_sem, xs_sem, xr_sem, ps_sem, pr_sem, ks_sem, kr_sem, rs_sem, rr_sem, os_sem, or_sem):
    n_outer, n_inner, tok, dm, g, hd, nb = dims
    n_row = n_inner // 2
    n_chips = n_outer * n_inner // 2
    rank = lax.axis_index("cpo") * n_inner + lax.axis_index("cpi")
    c = lax.div(rank, 2)
    h = lax.rem(rank, 2)
    oh = 1 - h

    def dev(chip, core):
        r = chip * 2 + core
        return {"cpo": lax.div(r, n_inner), "cpi": lax.rem(r, n_inner)}

    def load(src, dst, sem):
        cp = pltpu.make_async_copy(src, dst, sem)
        cp.start()
        return cp

    row, col = lax.div(c, n_row), lax.rem(c, n_row)
    n_rows = n_chips // n_row
    last = nb - 1


    barrier = pltpu.get_barrier_semaphore()

    def greet(chip, core):
        pl.semaphore_signal(barrier, inc=1, device_id=dev(chip, core), device_id_type=MESH)

    right = row * n_row + lax.rem(col + 1, n_row)
    left = row * n_row + lax.rem(col + n_row - 1, n_row)
    one = lambda cond: jnp.where(cond, 1, 0)
    both = jnp.logical_and
    up1, up2, dn1, dn2 = row + 1 < n_rows, row + 2 < n_rows, row >= 1, row >= 2

    odd = lax.rem(row, 2) == 1
    direct = [(up1, 4, c + 4), (col < 3, 1, c + 1), (col < 1, 3, c + 3), (col < 2, 2, c + 2), (both(up2, odd), 8, c + 8)]
    edge = lax.rem(row, 4) == 0
    later = [(both(up2, edge), 8, c + 8)]
    origin = [(dn1, c - 4), (col >= 1, c - 1), (both(dn2, jnp.logical_not(edge)), c - 8), (col >= 3, c - 3), (col >= 2, c - 2)]
    relay_row = [(dn1, 4, 5, right), (dn1, 4, 7, left), (both(dn1, both(up1, lax.rem(row, 4) == 3)), 4, 8, c + 4)]
    relay_far = [(both(dn2, col >= 1), 8, 3, left), (both(dn2, col == 3), 8, 1, right), (both(dn2, col >= 2), 8, 2, c - 2)]
    relay_5 = [(both(dn1, col < 2), 5, 6, right)]
    relay_7 = [(both(dn1, col < 2), 7, 6, left)]

    def when_all(cond, act):
        pl.when(cond)(act)

    greet(c, oh)
    for cond, chip in origin:
        when_all(cond, lambda chip=chip: [greet(chip, hh) for hh in range(2)] and None)
    when_all(dn1, lambda: [greet(chip, h) for chip in (left, right)] and None)
    when_all(both(dn2, col < 2), lambda: greet(c + 2, h))
    n_sent = 1 + 2 * one(dn1) + one(both(dn2, col >= 2))
    for cond, _, _ in direct + later:
        n_sent = n_sent + 2 * one(cond)

    ld_x = load(x_hbm, x2.at[h], ld_sem.at[0])
    ld_k = [load(wk_hbm.at[pl.ds(i * dm, dm)], wkr.at[pl.ds(i * dm, dm)], ld_sem.at[1 + i]) for i in range(2)]
    ld_v = [load(wv_hbm.at[pl.ds(i * dm, dm)], wvr.at[pl.ds(i * dm, dm)], ld_sem.at[6 + i]) for i in range(2)]
    ld_l = load(loc_hbm, loc, ld_sem.at[3])
    ld_b = load(bas_hbm, bas, ld_sem.at[4])
    def unpack(src, dst_row, rows):
        step = 1024

        def body(t, _):
            r = pl.multiple_of(t * step, step)
            big[pl.ds(pl.multiple_of(dst_row + r, step), step), :] = src[pl.ds(r, step), :].astype(F32)
            return 0

        lax.fori_loop(0, rows // step, body, 0)

    def columns(first, start, stride):
        return [big[pl.ds(first + s, dm, stride=stride), :].astype(BF16) for s in range(start, start + 2)]

    with jax.named_scope("relay_kv"):
        for ld in ld_k:
            ld.wait()
        unpack(wkr, 0, 2 * dm)
    ld_x.wait()
    with jax.named_scope("kvproj"):
        kp = jnp.dot(x2[h], jnp.concatenate(columns(0, 0, 2), axis=1), preferred_element_type=F32)
        for ld in ld_v:
            ld.wait()
        unpack(wvr, 2 * dm, 2 * dm)
        n_wq = wq_sem.shape[0]
        rows_wq = dm // n_wq
        head0 = pl.multiple_of(h * g, g)
        ld_q = [load(wq_hbm.at[pl.ds(i * rows_wq, rows_wq), pl.ds(head0, g), :], wqr.at[pl.ds(i * rows_wq, rows_wq)], wq_sem.at[i])
                for i in range(n_wq)]
        vp = jnp.dot(x2[h], jnp.concatenate(columns(2 * dm, 0, 2), axis=1), preferred_element_type=F32)
    ld_l.wait()
    ld_b.wait()
    t0 = pl.multiple_of(h * tok, tok)
    cb, sb = bas[0, pl.ds(c, 1), :], bas[1, pl.ds(c, 1), :]
    cl, sl = loc[0, pl.ds(t0, tok), :], loc[1, pl.ds(t0, tok), :]
    cos_k = cl * cb - sl * sb
    sin_k = sl * cb + cl * sb
    lane = lax.broadcasted_iota(jnp.int32, (tok, hd), 1)
    sin_k = jnp.where(lane < hd // 2, -sin_k, sin_k)
    for hh in range(2):
        k = kp[:, hh * hd:(hh + 1) * hd]
        k = (k * cos_k + pltpu.roll(k, hd // 2, 1) * sin_k).astype(BF16)
        v = vp[:, hh * hd:(hh + 1) * hd]
        own[hh, 0] = k
        own[hh, 1] = v.T.astype(BF16)
    kv[0, 0, h] = own[h, 0]
    kv[0, 1, h] = own[h, 1]

    with jax.named_scope("barrier"):
        pl.semaphore_wait(barrier, n_sent)
    x_copy = pltpu.make_async_remote_copy(src_ref=x2.at[h], dst_ref=x2.at[h], send_sem=xs_sem, recv_sem=xr_sem,
                                          device_id=dev(c, oh), device_id_type=MESH)

    p_copy = [pltpu.make_async_remote_copy(src_ref=own.at[oh, part], dst_ref=kv.at[0, part, h], send_sem=ps_sem.at[part], recv_sem=pr_sem.at[part],
                                           device_id=dev(c, oh), device_id_type=MESH) for part in range(2)]

    def each_direct(act, first, group):
        for i, (cond, slot, chip) in enumerate(group, first):
            @pl.when(cond)
            def _():
                for part in range(2):
                    for hh in range(2):
                        act(pltpu.make_async_remote_copy(src_ref=own.at[hh, part], dst_ref=kv.at[slot, part, h], send_sem=ks_sem.at[i, part, hh],
                                                         recv_sem=kr_sem.at[slot, part, h], device_id=dev(chip, hh), device_id_type=MESH))

    relays = relay_row + relay_far + relay_5 + relay_7

    def each_relay(act, group, part):
        for item in group:
            cond, src, dst, chip = item
            i = [r is item for r in relays].index(True)

            @pl.when(cond)
            def _():
                act(pltpu.make_async_remote_copy(src_ref=kv.at[src, part], dst_ref=kv.at[dst, part], send_sem=rs_sem.at[i, part],
                                                 recv_sem=rr_sem.at[dst, part], device_id=dev(chip, h), device_id_type=MESH))

    each_direct(lambda cp: cp.start(), 0, direct[:1])
    for cp in p_copy:
        cp.start()
    each_direct(lambda cp: cp.start(), 1, direct[1:])
    x_copy.start()

    ld_o = load(wo_hbm, wob, ld_sem.at[5])

    with jax.named_scope("relay_q"):
        dch = 128
        for i in range(n_wq):
            ld_q[i].wait()

            def unpack_q(t, _):
                d0 = pl.multiple_of(i * rows_wq + t * dch, dch)
                big[pl.ds(pl.multiple_of(d0 * g, dch * g), dch * g), :] = wqr[pl.ds(d0, dch)].astype(F32).reshape(dch * g, hd)
                return 0

            lax.fori_loop(0, rows_wq // dch, unpack_q, 0)
    each_direct(lambda cp: cp.start(), len(direct), later)
    half = hd // 2
    cl, sl = loc[0], loc[1]
    cs_t[0] = (cl * cb - sl * sb).T[:half]
    cs_t[1] = (sl * cb + cl * sb).T[:half]
    with jax.named_scope("xwait"):
        x_copy.wait_recv()
    xall = x2[...].reshape(2 * tok, dm)

    def proj_q(n):
        return jnp.dot(xall, jnp.concatenate(columns(0, 2 * n, g), axis=1), preferred_element_type=F32)

    with jax.named_scope("qproj"):
        for n in range(g // 2):
            qp = proj_q(n)
            for s in range(2):
                qt = qp[:, s * hd:(s + 1) * hd].T
                lo, hi = qt[:half], qt[half:]
                q_t[2 * n + s, :half] = (lo * cs_t[0] - hi * cs_t[1]).astype(BF16)
                q_t[2 * n + s, half:] = (hi * cs_t[0] + lo * cs_t[1]).astype(BF16)
    scale = hd ** -0.5 * math.log2(math.e)
    ki = lax.broadcasted_iota(jnp.int32, (2 * tok, 2 * tok), 0)
    qi = lax.broadcasted_iota(jnp.int32, (2 * tok, 2 * tok), 1)

    def attend(slot):
        kb = kv[slot, 0].reshape(2 * tok, hd)
        vb = jnp.concatenate([kv[slot, 1, 0], kv[slot, 1, 1]], axis=1)

        def weigh(n, s):
            if slot == 0:
                s = jnp.where(ki <= qi, s, -jnp.inf)
            if slot == last:
                s = jnp.where(ki > qi, s, -jnp.inf)
            top = jnp.max(s, axis=0, keepdims=True) * scale
            m_new = top if slot == 0 else jnp.maximum(m_s[n], top)
            p = jnp.exp2(s * scale - m_new)
            tot = jnp.sum(p, axis=0, keepdims=True)
            alpha = None
            if slot == 0:
                l_s[n] = tot
            else:
                alpha = jnp.exp2(m_s[n] - m_new)
                l_s[n] = l_s[n] * alpha + tot
            m_s[n] = m_new
            return p.astype(BF16), alpha

        def gather(n, p, alpha):
            r = jnp.dot(vb, p, preferred_element_type=F32)
            acc[n] = r if alpha is None else acc[n] * alpha + r

        scores, held = [], None
        for n in range(g):
            while len(scores) < min(n + 3, g):
                scores.append(jnp.dot(kb, q_t[len(scores)], preferred_element_type=F32))
            p, alpha = weigh(n, scores[n])
            if held is not None:
                gather(*held)
            held = (n, p, alpha)
        gather(*held)

    def landed(slot, relayed, group=(), parts=(0, 1)):
        for part in parts:
            with jax.named_scope(f"w{slot}{'kv'[part]}{'r' * relayed}"):
                if relayed:
                    pltpu.make_async_copy(kv.at[0, part], kv.at[slot, part], rr_sem.at[slot, part]).wait()
                else:
                    for s in range(2):
                        pltpu.make_async_copy(own.at[0, part], kv.at[slot, part, s], kr_sem.at[slot, part, s]).wait()
            each_relay(lambda cp: cp.start(), group, part)

    def visit(slot, here, relayed=False, got_if=None, group=()):
        @pl.when(here)
        def _():
            if got_if is None:
                landed(slot, relayed, group)
            elif got_if is edge:
                pl.when(edge)(lambda: landed(slot, True, group))
                pl.when(jnp.logical_not(edge))(lambda: landed(slot, False, group))
            elif got_if is not True:
                pl.when(jnp.logical_not(got_if))(lambda: landed(slot, relayed, group))
            with jax.named_scope(f"att{slot}"):
                attend(slot)

    pl.when(both(dn1, jnp.logical_not(edge)))(lambda: landed(4, False, relay_row, (0,)))
    with jax.named_scope("pwait"):
        for cp in p_copy:
            cp.wait_recv()
    with jax.named_scope("att0"):
        attend(0)
    pl.when(both(dn1, edge))(lambda: landed(4, False, relay_row, (0,)))
    pl.when(dn1)(lambda: landed(4, False, relay_row, (1,)))
    visit(4, dn1, got_if=True)
    visit(1, col >= 1)
    visit(8, dn2, got_if=edge, group=relay_far)

    @pl.when(both(dn1, col < 2))
    def _():
        for part in range(2):
            landed(5, True, relay_5, (part,))
            landed(7, True, relay_7, (part,))

    visit(2, col >= 2)
    visit(3, col >= 3)
    visit(5, dn1, relayed=True, got_if=col < 2)
    visit(7, dn1, relayed=True, got_if=col < 2)
    visit(3, both(dn2, col < 3), relayed=True)
    visit(6, dn1, relayed=True)
    visit(1, both(dn2, col < 1), relayed=True)
    visit(2, both(dn2, col < 2), relayed=True)

    def finish(n, _):
        o = (acc[n] / l_s[n]).T.astype(BF16)
        c0 = pl.multiple_of(n * hd, hd)
        o_send[0, :, pl.ds(c0, hd)] = o[:tok]
        o_send[1, :, pl.ds(c0, hd)] = o[tok:]
        return 0

    with jax.named_scope("finish"):
        lax.fori_loop(0, g, finish, 0, unroll=True)
    o_copy = pltpu.make_async_remote_copy(src_ref=o_send.at[oh], dst_ref=o_all, send_sem=os_sem, recv_sem=or_sem,
                                          device_id=dev(c, oh), device_id_type=MESH)
    o_copy.start()
    with jax.named_scope("wowait"):
        ld_o.wait()
    w0 = pl.multiple_of(h * g * hd, g * hd)
    w1 = pl.multiple_of(oh * g * hd, g * hd)
    o_own = o_send[h]
    n_y = 4
    cols = dm // n_y

    def own_part(i, _):
        c0 = pl.multiple_of(i * cols, cols)
        y_v[:, pl.ds(c0, cols)] = jnp.dot(o_own, wob[pl.ds(w0, g * hd), pl.ds(c0, cols)], preferred_element_type=F32)
        return 0

    with jax.named_scope("wo_own"):
        lax.fori_loop(0, n_y, own_part, 0, unroll=True)
    with jax.named_scope("owait"):
        o_copy.wait_recv()
    o_oth = o_all[...]
    with jax.named_scope("wo_oth"):
        for i in range(n_y):
            cs = slice(i * cols, (i + 1) * cols)
            y_ref[:, cs] = (y_v[:, cs] + jnp.dot(o_oth, wob[pl.ds(w1, g * hd), cs], preferred_element_type=F32)).astype(BF16)
    with jax.named_scope("sendwait"):
        x_copy.wait_send()
        for cp in p_copy:
            cp.wait_send()
        o_copy.wait_send()
        each_direct(lambda cp: cp.wait_send(), 0, direct + later)

        for part in range(2):
            each_relay(lambda cp: cp.wait_send(), relays, part)


def solution(mesh):
    n_outer, n_inner = mesh.shape['cpo'], mesh.shape['cpi']

    def local_fn(hidden, w_q, w_k, w_v, w_o):
        tok, dm = hidden.shape
        hq, hd = w_q.shape[1], w_q.shape[2]
        g = hq // 2
        nb = WINDOW // (2 * tok) + 1
        loc, bas = rope_tables(2 * tok, n_outer * n_inner // 2, hd)
        dims = (n_outer, n_inner, tok, dm, g, hd, nb)
        scratch = [
            pltpu.VMEM((2, tok, dm), BF16), pltpu.VMEM((dm, g, hd), BF16), pltpu.VMEM((2 * dm, hd), BF16), pltpu.VMEM((2 * dm, hd), BF16),
            pltpu.VMEM((dm * g, hd), F32), pltpu.VMEM((hq * hd, dm), BF16),
            pltpu.VMEM(loc.shape, F32), pltpu.VMEM(bas.shape, F32),
            pltpu.VMEM((2, 2, tok, hd), BF16), pltpu.VMEM((nb, 2, 2, tok, hd), BF16),
            pltpu.VMEM((g, hd, 2 * tok), BF16), pltpu.VMEM((2, hd // 2, 2 * tok), F32),
            pltpu.VMEM((g, 1, 2 * tok), F32), pltpu.VMEM((g, 1, 2 * tok), F32), pltpu.VMEM((g, hd, 2 * tok), F32),
            pltpu.VMEM((tok, g * hd), BF16), pltpu.VMEM((2, tok, g * hd), BF16), pltpu.VMEM((tok, dm), F32),
            pltpu.SemaphoreType.DMA((8,)), pltpu.SemaphoreType.DMA((4,)), pltpu.SemaphoreType.DMA, pltpu.SemaphoreType.DMA,
            pltpu.SemaphoreType.DMA((2,)), pltpu.SemaphoreType.DMA((2,)), pltpu.SemaphoreType.DMA((nb, 2, 2)), pltpu.SemaphoreType.DMA((nb, 2, 2)),
            pltpu.SemaphoreType.DMA((nb, 2)), pltpu.SemaphoreType.DMA((nb, 2)), pltpu.SemaphoreType.DMA, pltpu.SemaphoreType.DMA,
        ]
        return pl.pallas_call(
            functools.partial(kernel, dims),
            out_shape=pltpu.VMEM((tok, dm), BF16),
            in_specs=[pl.BlockSpec(memory_space=pl.ANY)] * 7,
            out_specs=pl.BlockSpec(memory_space=pltpu.VMEM),
            scratch_shapes=scratch,
            compiler_params=pltpu.CompilerParams(collective_id=0, has_side_effects=True, vmem_limit_bytes=56 * 1024 * 1024),
        )(hidden, w_q, w_k.reshape(2 * dm, hd), w_v.reshape(2 * dm, hd), w_o.reshape(hq * hd, dm), jnp.asarray(loc), jnp.asarray(bas))

    return jax.shard_map(local_fn, mesh=mesh,
                         in_specs=(P(('dp', 'cpo', 'cpi'), None), P(), P(), P(), P()),
                         out_specs=P(('dp', 'cpo', 'cpi'), None), check_vma=False)
```

```python
import functools
import math

import jax
import jax.numpy as jnp
import numpy as np
from jax import lax
from jax.experimental import pallas as pl
from jax.experimental.pallas import tpu as pltpu
from jax.sharding import PartitionSpec as P

WINDOW = 2048
ROPE_BASE = 10000.0
MESH = pl.DeviceIdType.MESH
F32, BF16 = jnp.float32, jnp.bfloat16


def rope_tables(tok_chip, n_chips, head_dim):
    half = head_dim // 2
    freq = ROPE_BASE ** (-np.arange(half, dtype=np.float64) * 2.0 / head_dim)
    local = np.arange(tok_chip, dtype=np.float64)[:, None] * freq
    base = (np.arange(n_chips, dtype=np.float64) * tok_chip)[:, None] * freq
    dup = lambda a: np.concatenate([a, a], axis=-1)
    loc = np.stack([dup(np.cos(local)), dup(np.sin(local))]).astype(np.float32)
    bas = np.stack([dup(np.cos(base)), dup(np.sin(base))]).astype(np.float32)
    return loc, bas


def kernel(dims, x_hbm, wq_hbm, wk_hbm, wv_hbm, wo_hbm, loc_hbm, bas_hbm, y_ref,
           x2, wqr, wkr, wvr, big, wob, loc, bas, own, kv, q_t, cs_t, m_s, l_s, acc, o_all, o_send, y_v,
           ld_sem, wq_sem, xs_sem, xr_sem, ps_sem, pr_sem, ks_sem, kr_sem, rs_sem, rr_sem, os_sem, or_sem):
    n_outer, n_inner, tok, dm, g, hd, nb = dims
    n_row = n_inner // 2
    n_chips = n_outer * n_inner // 2
    rank = lax.axis_index("cpo") * n_inner + lax.axis_index("cpi")
    c = lax.div(rank, 2)
    h = lax.rem(rank, 2)
    oh = 1 - h

    def dev(chip, core):
        r = chip * 2 + core
        return {"cpo": lax.div(r, n_inner), "cpi": lax.rem(r, n_inner)}

    def load(src, dst, sem):
        cp = pltpu.make_async_copy(src, dst, sem)
        cp.start()
        return cp

    row, col = lax.div(c, n_row), lax.rem(c, n_row)
    n_rows = n_chips // n_row
    last = nb - 1


    barrier = pltpu.get_barrier_semaphore()

    def greet(chip, core):
        pl.semaphore_signal(barrier, inc=1, device_id=dev(chip, core), device_id_type=MESH)

    right = row * n_row + lax.rem(col + 1, n_row)
    left = row * n_row + lax.rem(col + n_row - 1, n_row)
    one = lambda cond: jnp.where(cond, 1, 0)
    both = jnp.logical_and
    up1, up2, dn1, dn2 = row + 1 < n_rows, row + 2 < n_rows, row >= 1, row >= 2

    odd = lax.rem(row, 2) == 1
    direct = [(up1, 4, c + 4), (col < 3, 1, c + 1), (col < 1, 3, c + 3), (col < 2, 2, c + 2), (both(up2, odd), 8, c + 8)]
    edge = lax.rem(row, 4) == 0
    later = [(both(up2, edge), 8, c + 8)]
    origin = [(dn1, c - 4), (col >= 1, c - 1), (both(dn2, jnp.logical_not(edge)), c - 8), (col >= 3, c - 3), (col >= 2, c - 2)]
    relay_row = [(dn1, 4, 5, right), (dn1, 4, 7, left), (both(dn1, both(up1, lax.rem(row, 4) == 3)), 4, 8, c + 4)]
    relay_far = [(both(dn2, col >= 1), 8, 3, left), (both(dn2, col == 3), 8, 1, right), (both(dn2, col >= 2), 8, 2, c - 2)]
    relay_5 = [(both(dn1, col < 2), 5, 6, right)]
    relay_7 = [(both(dn1, col < 2), 7, 6, left)]

    def when_all(cond, act):
        pl.when(cond)(act)

    greet(c, oh)
    for cond, chip in origin:
        when_all(cond, lambda chip=chip: [greet(chip, hh) for hh in range(2)] and None)
    when_all(dn1, lambda: [greet(chip, h) for chip in (left, right)] and None)
    when_all(both(dn2, col < 2), lambda: greet(c + 2, h))
    n_sent = 1 + 2 * one(dn1) + one(both(dn2, col >= 2))
    for cond, _, _ in direct + later:
        n_sent = n_sent + 2 * one(cond)

    ld_x = load(x_hbm, x2.at[h], ld_sem.at[0])
    ld_k = [load(wk_hbm.at[pl.ds(i * dm, dm)], wkr.at[pl.ds(i * dm, dm)], ld_sem.at[1 + i]) for i in range(2)]
    ld_v = [load(wv_hbm.at[pl.ds(i * dm, dm)], wvr.at[pl.ds(i * dm, dm)], ld_sem.at[6 + i]) for i in range(2)]
    ld_l = load(loc_hbm, loc, ld_sem.at[3])
    ld_b = load(bas_hbm, bas, ld_sem.at[4])
    def unpack(src, dst_row, rows):
        step = 1024

        def body(t, _):
            r = pl.multiple_of(t * step, step)
            big[pl.ds(pl.multiple_of(dst_row + r, step), step), :] = src[pl.ds(r, step), :].astype(F32)
            return 0

        lax.fori_loop(0, rows // step, body, 0)

    def columns(first, start, stride):
        return [big[pl.ds(first + s, dm, stride=stride), :].astype(BF16) for s in range(start, start + 2)]

    with jax.named_scope("relay_kv"):
        for ld in ld_k:
            ld.wait()
        unpack(wkr, 0, 2 * dm)
    ld_x.wait()
    with jax.named_scope("kvproj"):
        kp = jnp.dot(x2[h], jnp.concatenate(columns(0, 0, 2), axis=1), preferred_element_type=F32)
        for ld in ld_v:
            ld.wait()
        unpack(wvr, 2 * dm, 2 * dm)
        n_wq = wq_sem.shape[0]
        rows_wq = dm // n_wq
        head0 = pl.multiple_of(h * g, g)
        ld_q = [load(wq_hbm.at[pl.ds(i * rows_wq, rows_wq), pl.ds(head0, g), :], wqr.at[pl.ds(i * rows_wq, rows_wq)], wq_sem.at[i])
                for i in range(n_wq)]
        vp = jnp.dot(x2[h], jnp.concatenate(columns(2 * dm, 0, 2), axis=1), preferred_element_type=F32)
    ld_l.wait()
    ld_b.wait()
    t0 = pl.multiple_of(h * tok, tok)
    cb, sb = bas[0, pl.ds(c, 1), :], bas[1, pl.ds(c, 1), :]
    cl, sl = loc[0, pl.ds(t0, tok), :], loc[1, pl.ds(t0, tok), :]
    cos_k = cl * cb - sl * sb
    sin_k = sl * cb + cl * sb
    lane = lax.broadcasted_iota(jnp.int32, (tok, hd), 1)
    sin_k = jnp.where(lane < hd // 2, -sin_k, sin_k)
    for hh in range(2):
        k = kp[:, hh * hd:(hh + 1) * hd]
        k = (k * cos_k + pltpu.roll(k, hd // 2, 1) * sin_k).astype(BF16)
        v = vp[:, hh * hd:(hh + 1) * hd]
        own[hh, 0] = k
        own[hh, 1] = v.T.astype(BF16)
    kv[0, 0, h] = own[h, 0]
    kv[0, 1, h] = own[h, 1]

    with jax.named_scope("barrier"):
        pl.semaphore_wait(barrier, n_sent)
    x_copy = pltpu.make_async_remote_copy(src_ref=x2.at[h], dst_ref=x2.at[h], send_sem=xs_sem, recv_sem=xr_sem,
                                          device_id=dev(c, oh), device_id_type=MESH)

    p_copy = [pltpu.make_async_remote_copy(src_ref=own.at[oh, part], dst_ref=kv.at[0, part, h], send_sem=ps_sem.at[part], recv_sem=pr_sem.at[part],
                                           device_id=dev(c, oh), device_id_type=MESH) for part in range(2)]

    def each_direct(act, first, group):
        for i, (cond, slot, chip) in enumerate(group, first):
            @pl.when(cond)
            def _():
                for part in range(2):
                    for hh in range(2):
                        act(pltpu.make_async_remote_copy(src_ref=own.at[hh, part], dst_ref=kv.at[slot, part, h], send_sem=ks_sem.at[i, part, hh],
                                                         recv_sem=kr_sem.at[slot, part, h], device_id=dev(chip, hh), device_id_type=MESH))

    relays = relay_row + relay_far + relay_5 + relay_7

    def each_relay(act, group, part):
        for item in group:
            cond, src, dst, chip = item
            i = [r is item for r in relays].index(True)

            @pl.when(cond)
            def _():
                act(pltpu.make_async_remote_copy(src_ref=kv.at[src, part], dst_ref=kv.at[dst, part], send_sem=rs_sem.at[i, part],
                                                 recv_sem=rr_sem.at[dst, part], device_id=dev(chip, h), device_id_type=MESH))

    each_direct(lambda cp: cp.start(), 0, direct[:1])
    for cp in p_copy:
        cp.start()
    each_direct(lambda cp: cp.start(), 1, direct[1:])
    x_copy.start()

    ld_o = load(wo_hbm, wob, ld_sem.at[5])

    with jax.named_scope("relay_q"):
        dch = 128
        for i in range(n_wq):
            ld_q[i].wait()

            def unpack_q(t, _):
                d0 = pl.multiple_of(i * rows_wq + t * dch, dch)
                big[pl.ds(pl.multiple_of(d0 * g, dch * g), dch * g), :] = wqr[pl.ds(d0, dch)].astype(F32).reshape(dch * g, hd)
                return 0

            lax.fori_loop(0, rows_wq // dch, unpack_q, 0)
    each_direct(lambda cp: cp.start(), len(direct), later)
    half = hd // 2
    cl, sl = loc[0], loc[1]
    cs_t[0] = (cl * cb - sl * sb).T[:half]
    cs_t[1] = (sl * cb + cl * sb).T[:half]
    with jax.named_scope("xwait"):
        x_copy.wait_recv()
    xall = x2[...].reshape(2 * tok, dm)

    def proj_q(n):
        return jnp.dot(xall, jnp.concatenate(columns(0, 2 * n, g), axis=1), preferred_element_type=F32)

    with jax.named_scope("qproj"):
        for n in range(g // 2):
            qp = proj_q(n)
            for s in range(2):
                qt = qp[:, s * hd:(s + 1) * hd].T
                lo, hi = qt[:half], qt[half:]
                q_t[2 * n + s, :half] = (lo * cs_t[0] - hi * cs_t[1]).astype(BF16)
                q_t[2 * n + s, half:] = (hi * cs_t[0] + lo * cs_t[1]).astype(BF16)
    scale = hd ** -0.5 * math.log2(math.e)
    ki = lax.broadcasted_iota(jnp.int32, (2 * tok, 2 * tok), 0)
    qi = lax.broadcasted_iota(jnp.int32, (2 * tok, 2 * tok), 1)

    def attend(slot):
        kb = kv[slot, 0].reshape(2 * tok, hd)
        vb = jnp.concatenate([kv[slot, 1, 0], kv[slot, 1, 1]], axis=1)

        def weigh(n, s):
            if slot == 0:
                s = jnp.where(ki <= qi, s, -jnp.inf)
            if slot == last:
                s = jnp.where(ki > qi, s, -jnp.inf)
            top = jnp.max(s, axis=0, keepdims=True) * scale
            m_new = top if slot == 0 else jnp.maximum(m_s[n], top)
            p = jnp.exp2(s * scale - m_new)
            tot = jnp.sum(p, axis=0, keepdims=True)
            alpha = None
            if slot == 0:
                l_s[n] = tot
            else:
                alpha = jnp.exp2(m_s[n] - m_new)
                l_s[n] = l_s[n] * alpha + tot
            m_s[n] = m_new
            return p.astype(BF16), alpha

        def gather(n, p, alpha):
            r = jnp.dot(vb, p, preferred_element_type=F32)
            acc[n] = r if alpha is None else acc[n] * alpha + r

        scores, held = [], []
        for n in range(g):
            while len(scores) < min(n + 5, g):
                scores.append(jnp.dot(kb, q_t[len(scores)], preferred_element_type=F32))
            held.append((n, *weigh(n, scores[n])))
            if len(held) > 3:
                gather(*held.pop(0))
        for item in held:
            gather(*item)

    def landed(slot, relayed, group=(), parts=(0, 1)):
        for part in parts:
            with jax.named_scope(f"w{slot}{'kv'[part]}{'r' * relayed}"):
                if relayed:
                    pltpu.make_async_copy(kv.at[0, part], kv.at[slot, part], rr_sem.at[slot, part]).wait()
                else:
                    for s in range(2):
                        pltpu.make_async_copy(own.at[0, part], kv.at[slot, part, s], kr_sem.at[slot, part, s]).wait()
            each_relay(lambda cp: cp.start(), group, part)

    def visit(slot, here, relayed=False, got_if=None, group=()):
        @pl.when(here)
        def _():
            if got_if is None:
                landed(slot, relayed, group)
            elif got_if is not True:
                pl.when(jnp.logical_not(got_if))(lambda: landed(slot, relayed, group))
            with jax.named_scope(f"att{slot}"):
                attend(slot)

    pl.when(both(dn1, jnp.logical_not(edge)))(lambda: landed(4, False, relay_row, (0,)))
    with jax.named_scope("pwait"):
        for cp in p_copy:
            cp.wait_recv()
    with jax.named_scope("att0"):
        attend(0)
    pl.when(both(dn1, edge))(lambda: landed(4, False, relay_row, (0,)))
    pl.when(dn1)(lambda: landed(4, False, relay_row, (1,)))
    visit(4, dn1, got_if=True)
    visit(1, col >= 1)
    slow = both(edge, col < 2)

    @pl.when(both(dn2, jnp.logical_not(edge)))
    def _():
        landed(8, False, relay_far)

    @pl.when(both(dn2, edge))
    def _():
        landed(8, True, relay_far, (0,))

        @pl.when(col < 2)
        def _():
            landed(5, True, relay_5, (0,))
            landed(7, True, relay_7, (0,))
        landed(8, True, relay_far, (1,))

    visit(8, dn2, got_if=True)

    @pl.when(both(dn1, col < 2))
    def _():
        @pl.when(jnp.logical_not(slow))
        def _():
            landed(5, True, relay_5, (0,))
            landed(7, True, relay_7, (0,))
        landed(5, True, relay_5, (1,))
        landed(7, True, relay_7, (1,))

    visit(2, col >= 2)
    visit(3, col >= 3)
    visit(5, dn1, relayed=True, got_if=col < 2)
    visit(7, dn1, relayed=True, got_if=col < 2)
    visit(3, both(dn2, col < 3), relayed=True)
    visit(6, dn1, relayed=True)
    visit(2, both(dn2, col < 2), relayed=True)
    visit(1, both(dn2, col < 1), relayed=True)

    def finish(n, _):
        o = (acc[n] / l_s[n]).T.astype(BF16)
        c0 = pl.multiple_of(n * hd, hd)
        o_send[0, :, pl.ds(c0, hd)] = o[:tok]
        o_send[1, :, pl.ds(c0, hd)] = o[tok:]
        return 0

    with jax.named_scope("finish"):
        lax.fori_loop(0, g, finish, 0, unroll=True)
    o_copy = pltpu.make_async_remote_copy(src_ref=o_send.at[oh], dst_ref=o_all, send_sem=os_sem, recv_sem=or_sem,
                                          device_id=dev(c, oh), device_id_type=MESH)
    o_copy.start()
    with jax.named_scope("wowait"):
        ld_o.wait()
    w0 = pl.multiple_of(h * g * hd, g * hd)
    w1 = pl.multiple_of(oh * g * hd, g * hd)
    o_own = o_send[h]
    n_y = 4
    cols = dm // n_y

    def own_part(i, _):
        c0 = pl.multiple_of(i * cols, cols)
        y_v[:, pl.ds(c0, cols)] = jnp.dot(o_own, wob[pl.ds(w0, g * hd), pl.ds(c0, cols)], preferred_element_type=F32)
        return 0

    with jax.named_scope("wo_own"):
        lax.fori_loop(0, n_y, own_part, 0, unroll=True)
    with jax.named_scope("owait"):
        o_copy.wait_recv()
    o_oth = o_all[...]
    with jax.named_scope("wo_oth"):
        for i in range(n_y):
            cs = slice(i * cols, (i + 1) * cols)
            y_ref[:, cs] = (y_v[:, cs] + jnp.dot(o_oth, wob[pl.ds(w1, g * hd), cs], preferred_element_type=F32)).astype(BF16)
    with jax.named_scope("sendwait"):
        x_copy.wait_send()
        for cp in p_copy:
            cp.wait_send()
        o_copy.wait_send()
        each_direct(lambda cp: cp.wait_send(), 0, direct + later)

        for part in range(2):
            each_relay(lambda cp: cp.wait_send(), relays, part)


def solution(mesh):
    n_outer, n_inner = mesh.shape['cpo'], mesh.shape['cpi']

    def local_fn(hidden, w_q, w_k, w_v, w_o):
        tok, dm = hidden.shape
        hq, hd = w_q.shape[1], w_q.shape[2]
        g = hq // 2
        nb = WINDOW // (2 * tok) + 1
        loc, bas = rope_tables(2 * tok, n_outer * n_inner // 2, hd)
        dims = (n_outer, n_inner, tok, dm, g, hd, nb)
        scratch = [
            pltpu.VMEM((2, tok, dm), BF16), pltpu.VMEM((dm, g, hd), BF16), pltpu.VMEM((2 * dm, hd), BF16), pltpu.VMEM((2 * dm, hd), BF16),
            pltpu.VMEM((dm * g, hd), F32), pltpu.VMEM((hq * hd, dm), BF16),
            pltpu.VMEM(loc.shape, F32), pltpu.VMEM(bas.shape, F32),
            pltpu.VMEM((2, 2, tok, hd), BF16), pltpu.VMEM((nb, 2, 2, tok, hd), BF16),
            pltpu.VMEM((g, hd, 2 * tok), BF16), pltpu.VMEM((2, hd // 2, 2 * tok), F32),
            pltpu.VMEM((g, 1, 2 * tok), F32), pltpu.VMEM((g, 1, 2 * tok), F32), pltpu.VMEM((g, hd, 2 * tok), F32),
            pltpu.VMEM((tok, g * hd), BF16), pltpu.VMEM((2, tok, g * hd), BF16), pltpu.VMEM((tok, dm), F32),
            pltpu.SemaphoreType.DMA((8,)), pltpu.SemaphoreType.DMA((4,)), pltpu.SemaphoreType.DMA, pltpu.SemaphoreType.DMA,
            pltpu.SemaphoreType.DMA((2,)), pltpu.SemaphoreType.DMA((2,)), pltpu.SemaphoreType.DMA((nb, 2, 2)), pltpu.SemaphoreType.DMA((nb, 2, 2)),
            pltpu.SemaphoreType.DMA((nb, 2)), pltpu.SemaphoreType.DMA((nb, 2)), pltpu.SemaphoreType.DMA, pltpu.SemaphoreType.DMA,
        ]
        return pl.pallas_call(
            functools.partial(kernel, dims),
            out_shape=pltpu.VMEM((tok, dm), BF16),
            in_specs=[pl.BlockSpec(memory_space=pl.ANY)] * 7,
            out_specs=pl.BlockSpec(memory_space=pltpu.VMEM),
            scratch_shapes=scratch,
            compiler_params=pltpu.CompilerParams(collective_id=0, has_side_effects=True, vmem_limit_bytes=56 * 1024 * 1024),
        )(hidden, w_q, w_k.reshape(2 * dm, hd), w_v.reshape(2 * dm, hd), w_o.reshape(hq * hd, dm), jnp.asarray(loc), jnp.asarray(bas))

    return jax.shard_map(local_fn, mesh=mesh,
                         in_specs=(P(('dp', 'cpo', 'cpi'), None), P(), P(), P(), P()),
                         out_specs=P(('dp', 'cpo', 'cpi'), None), check_vma=False)
```

```python
import functools
import math

import jax
import jax.numpy as jnp
import numpy as np
from jax import lax
from jax.experimental import pallas as pl
from jax.experimental.pallas import tpu as pltpu
from jax.sharding import PartitionSpec as P

WINDOW = 2048
ROPE_BASE = 10000.0
MESH = pl.DeviceIdType.MESH
F32, BF16 = jnp.float32, jnp.bfloat16


def rope_tables(tok_chip, n_chips, head_dim):
    half = head_dim // 2
    freq = ROPE_BASE ** (-np.arange(half, dtype=np.float64) * 2.0 / head_dim)
    local = np.arange(tok_chip, dtype=np.float64)[:, None] * freq
    base = (np.arange(n_chips, dtype=np.float64) * tok_chip)[:, None] * freq
    dup = lambda a: np.concatenate([a, a], axis=-1)
    loc = np.stack([dup(np.cos(local)), dup(np.sin(local))]).astype(np.float32)
    bas = np.stack([dup(np.cos(base)), dup(np.sin(base))]).astype(np.float32)
    return loc, bas


def kernel(dims, x_hbm, wq_hbm, wk_hbm, wv_hbm, wo_hbm, loc_hbm, bas_hbm, y_ref,
           x2, wqr, wkr, wvr, big, wob, loc, bas, own, kv, q_t, cs_t, m_s, l_s, acc, o_all, o_send, y_v,
           ld_sem, wq_sem, xs_sem, xr_sem, ps_sem, pr_sem, ks_sem, kr_sem, rs_sem, rr_sem, os_sem, or_sem):
    n_outer, n_inner, tok, dm, g, hd, nb = dims
    n_row = n_inner // 2
    n_chips = n_outer * n_inner // 2
    rank = lax.axis_index("cpo") * n_inner + lax.axis_index("cpi")
    c = lax.div(rank, 2)
    h = lax.rem(rank, 2)
    oh = 1 - h

    def dev(chip, core):
        r = chip * 2 + core
        return {"cpo": lax.div(r, n_inner), "cpi": lax.rem(r, n_inner)}

    def load(src, dst, sem):
        cp = pltpu.make_async_copy(src, dst, sem)
        cp.start()
        return cp

    row, col = lax.div(c, n_row), lax.rem(c, n_row)
    n_rows = n_chips // n_row
    last = nb - 1


    barrier = pltpu.get_barrier_semaphore()

    def greet(chip, core):
        pl.semaphore_signal(barrier, inc=1, device_id=dev(chip, core), device_id_type=MESH)

    right = row * n_row + lax.rem(col + 1, n_row)
    left = row * n_row + lax.rem(col + n_row - 1, n_row)
    one = lambda cond: jnp.where(cond, 1, 0)
    both = jnp.logical_and
    up1, up2, dn1, dn2 = row + 1 < n_rows, row + 2 < n_rows, row >= 1, row >= 2

    odd = lax.rem(row, 2) == 1
    direct = [(up1, 4, c + 4), (col < 3, 1, c + 1), (col < 1, 3, c + 3), (col < 2, 2, c + 2), (both(up2, odd), 8, c + 8)]
    edge = lax.rem(row, 4) == 0
    later = [(both(up2, edge), 8, c + 8)]
    origin = [(dn1, c - 4), (col >= 1, c - 1), (both(dn2, jnp.logical_not(edge)), c - 8), (col >= 3, c - 3), (col >= 2, c - 2)]
    relay_row = [(both(dn1, both(up1, lax.rem(row, 4) == 3)), 4, 8, c + 4), (dn1, 4, 5, right), (dn1, 4, 7, left)]
    relay_far = [(both(dn2, col >= 1), 8, 3, left), (both(dn2, col == 3), 8, 1, right), (both(dn2, col >= 2), 8, 2, c - 2)]
    relay_5 = [(both(dn1, col < 2), 5, 6, right)]
    relay_7 = [(both(dn1, col < 2), 7, 6, left)]

    def when_all(cond, act):
        pl.when(cond)(act)

    greet(c, oh)
    for cond, chip in origin:
        when_all(cond, lambda chip=chip: [greet(chip, hh) for hh in range(2)] and None)
    when_all(dn1, lambda: [greet(chip, h) for chip in (left, right)] and None)
    when_all(both(dn2, col < 2), lambda: greet(c + 2, h))
    n_sent = 1 + 2 * one(dn1) + one(both(dn2, col >= 2))
    for cond, _, _ in direct + later:
        n_sent = n_sent + 2 * one(cond)

    ld_x = load(x_hbm, x2.at[h], ld_sem.at[0])
    ld_k = [load(wk_hbm.at[pl.ds(i * dm, dm)], wkr.at[pl.ds(i * dm, dm)], ld_sem.at[1 + i]) for i in range(2)]
    ld_v = [load(wv_hbm.at[pl.ds(i * dm, dm)], wvr.at[pl.ds(i * dm, dm)], ld_sem.at[6 + i]) for i in range(2)]
    ld_l = load(loc_hbm, loc, ld_sem.at[3])
    ld_b = load(bas_hbm, bas, ld_sem.at[4])
    def unpack(src, dst_row, rows):
        step = 1024

        def body(t, _):
            r = pl.multiple_of(t * step, step)
            big[pl.ds(pl.multiple_of(dst_row + r, step), step), :] = src[pl.ds(r, step), :].astype(F32)
            return 0

        lax.fori_loop(0, rows // step, body, 0)

    def columns(first, start, stride):
        return [big[pl.ds(first + s, dm, stride=stride), :].astype(BF16) for s in range(start, start + 2)]

    with jax.named_scope("relay_kv"):
        for ld in ld_k:
            ld.wait()
        unpack(wkr, 0, 2 * dm)
    ld_x.wait()
    with jax.named_scope("kvproj"):
        kp = jnp.dot(x2[h], jnp.concatenate(columns(0, 0, 2), axis=1), preferred_element_type=F32)
        for ld in ld_v:
            ld.wait()
        unpack(wvr, 2 * dm, 2 * dm)
        n_wq = wq_sem.shape[0]
        rows_wq = dm // n_wq
        head0 = pl.multiple_of(h * g, g)
        ld_q = [load(wq_hbm.at[pl.ds(i * rows_wq, rows_wq), pl.ds(head0, g), :], wqr.at[pl.ds(i * rows_wq, rows_wq)], wq_sem.at[i])
                for i in range(n_wq)]
        vp = jnp.dot(x2[h], jnp.concatenate(columns(2 * dm, 0, 2), axis=1), preferred_element_type=F32)
    ld_l.wait()
    ld_b.wait()
    t0 = pl.multiple_of(h * tok, tok)
    cb, sb = bas[0, pl.ds(c, 1), :], bas[1, pl.ds(c, 1), :]
    cl, sl = loc[0, pl.ds(t0, tok), :], loc[1, pl.ds(t0, tok), :]
    cos_k = cl * cb - sl * sb
    sin_k = sl * cb + cl * sb
    lane = lax.broadcasted_iota(jnp.int32, (tok, hd), 1)
    sin_k = jnp.where(lane < hd // 2, -sin_k, sin_k)
    for hh in range(2):
        k = kp[:, hh * hd:(hh + 1) * hd]
        k = (k * cos_k + pltpu.roll(k, hd // 2, 1) * sin_k).astype(BF16)
        v = vp[:, hh * hd:(hh + 1) * hd]
        own[hh, 0] = k
        own[hh, 1] = v.T.astype(BF16)
    kv[0, 0, h] = own[h, 0]
    kv[0, 1, h] = own[h, 1]

    with jax.named_scope("barrier"):
        pl.semaphore_wait(barrier, n_sent)
    x_copy = pltpu.make_async_remote_copy(src_ref=x2.at[h], dst_ref=x2.at[h], send_sem=xs_sem, recv_sem=xr_sem,
                                          device_id=dev(c, oh), device_id_type=MESH)

    p_copy = [pltpu.make_async_remote_copy(src_ref=own.at[oh, part], dst_ref=kv.at[0, part, h], send_sem=ps_sem.at[part], recv_sem=pr_sem.at[part],
                                           device_id=dev(c, oh), device_id_type=MESH) for part in range(2)]

    def each_direct(act, first, group):
        for i, (cond, slot, chip) in enumerate(group, first):
            @pl.when(cond)
            def _():
                for part in range(2):
                    for hh in range(2):
                        act(pltpu.make_async_remote_copy(src_ref=own.at[hh, part], dst_ref=kv.at[slot, part, h], send_sem=ks_sem.at[i, part, hh],
                                                         recv_sem=kr_sem.at[slot, part, h], device_id=dev(chip, hh), device_id_type=MESH))

    relays = relay_row + relay_far + relay_5 + relay_7

    def each_relay(act, group, part):
        for item in group:
            cond, src, dst, chip = item
            i = [r is item for r in relays].index(True)

            @pl.when(cond)
            def _():
                act(pltpu.make_async_remote_copy(src_ref=kv.at[src, part], dst_ref=kv.at[dst, part], send_sem=rs_sem.at[i, part],
                                                 recv_sem=rr_sem.at[dst, part], device_id=dev(chip, h), device_id_type=MESH))

    each_direct(lambda cp: cp.start(), 0, direct[:1])
    for cp in p_copy:
        cp.start()
    each_direct(lambda cp: cp.start(), 1, direct[1:])
    x_copy.start()

    ld_o = load(wo_hbm, wob, ld_sem.at[5])

    with jax.named_scope("relay_q"):
        dch = 128
        for i in range(n_wq):
            ld_q[i].wait()

            def unpack_q(t, _):
                d0 = pl.multiple_of(i * rows_wq + t * dch, dch)
                big[pl.ds(pl.multiple_of(d0 * g, dch * g), dch * g), :] = wqr[pl.ds(d0, dch)].astype(F32).reshape(dch * g, hd)
                return 0

            lax.fori_loop(0, rows_wq // dch, unpack_q, 0)
    each_direct(lambda cp: cp.start(), len(direct), later)
    half = hd // 2
    cl, sl = loc[0], loc[1]
    cs_t[0] = (cl * cb - sl * sb).T[:half]
    cs_t[1] = (sl * cb + cl * sb).T[:half]
    with jax.named_scope("xwait"):
        x_copy.wait_recv()
    xall = x2[...].reshape(2 * tok, dm)

    def proj_q(n):
        return jnp.dot(xall, jnp.concatenate(columns(0, 2 * n, g), axis=1), preferred_element_type=F32)

    with jax.named_scope("qproj"):
        for n in range(g // 2):
            qp = proj_q(n)
            for s in range(2):
                qt = qp[:, s * hd:(s + 1) * hd].T
                lo, hi = qt[:half], qt[half:]
                q_t[2 * n + s, :half] = (lo * cs_t[0] - hi * cs_t[1]).astype(BF16)
                q_t[2 * n + s, half:] = (hi * cs_t[0] + lo * cs_t[1]).astype(BF16)
    scale = hd ** -0.5 * math.log2(math.e)
    ki = lax.broadcasted_iota(jnp.int32, (2 * tok, 2 * tok), 0)
    qi = lax.broadcasted_iota(jnp.int32, (2 * tok, 2 * tok), 1)

    def attend(slot):
        kb = kv[slot, 0].reshape(2 * tok, hd)
        vb = jnp.concatenate([kv[slot, 1, 0], kv[slot, 1, 1]], axis=1)

        def weigh(n, s):
            if slot == 0:
                s = jnp.where(ki <= qi, s, -jnp.inf)
            if slot == last:
                s = jnp.where(ki > qi, s, -jnp.inf)
            top = jnp.max(s, axis=0, keepdims=True) * scale
            m_new = top if slot == 0 else jnp.maximum(m_s[n], top)
            p = jnp.exp2(s * scale - m_new)
            tot = jnp.sum(p, axis=0, keepdims=True)
            alpha = None
            if slot == 0:
                l_s[n] = tot
            else:
                alpha = jnp.exp2(m_s[n] - m_new)
                l_s[n] = l_s[n] * alpha + tot
            m_s[n] = m_new
            return p.astype(BF16), alpha

        def gather(n, p, alpha):
            r = jnp.dot(vb, p, preferred_element_type=F32)
            acc[n] = r if alpha is None else acc[n] * alpha + r

        scores, held = [], []
        for n in range(g):
            while len(scores) < min(n + 5, g):
                scores.append(jnp.dot(kb, q_t[len(scores)], preferred_element_type=F32))
            held.append((n, *weigh(n, scores[n])))
            if len(held) > 3:
                gather(*held.pop(0))
        for item in held:
            gather(*item)

    def landed(slot, relayed, group=(), parts=(0, 1)):
        for part in parts:
            with jax.named_scope(f"w{slot}{'kv'[part]}{'r' * relayed}"):
                if relayed:
                    pltpu.make_async_copy(kv.at[0, part], kv.at[slot, part], rr_sem.at[slot, part]).wait()
                else:
                    for s in range(2):
                        pltpu.make_async_copy(own.at[0, part], kv.at[slot, part, s], kr_sem.at[slot, part, s]).wait()
            each_relay(lambda cp: cp.start(), group, part)

    def visit(slot, here, relayed=False, got_if=None, group=()):
        @pl.when(here)
        def _():
            if got_if is None:
                landed(slot, relayed, group)
            elif got_if is not True:
                pl.when(jnp.logical_not(got_if))(lambda: landed(slot, relayed, group))
            with jax.named_scope(f"att{slot}"):
                attend(slot)

    pl.when(both(dn1, jnp.logical_not(edge)))(lambda: landed(4, False, relay_row, (0,)))
    with jax.named_scope("pwait"):
        for cp in p_copy:
            cp.wait_recv()
    with jax.named_scope("att0"):
        attend(0)
    pl.when(both(dn1, edge))(lambda: landed(4, False, relay_row, (0,)))
    pl.when(dn1)(lambda: landed(4, False, relay_row, (1,)))
    visit(4, dn1, got_if=True)
    visit(1, col >= 1)
    slow = both(edge, col < 2)

    @pl.when(both(dn2, jnp.logical_not(edge)))
    def _():
        landed(8, False, relay_far)

    @pl.when(both(dn2, edge))
    def _():
        landed(8, True, relay_far, (0,))

        @pl.when(col < 2)
        def _():
            landed(5, True, relay_5, (0,))
            landed(7, True, relay_7, (0,))
        landed(8, True, relay_far, (1,))

    visit(8, dn2, got_if=True)

    @pl.when(both(dn1, col < 2))
    def _():
        @pl.when(jnp.logical_not(slow))
        def _():
            landed(5, True, relay_5, (0,))
            landed(7, True, relay_7, (0,))
        landed(5, True, relay_5, (1,))
        landed(7, True, relay_7, (1,))

    visit(2, col >= 2)
    visit(3, col >= 3)
    visit(5, dn1, relayed=True, got_if=col < 2)
    visit(7, dn1, relayed=True, got_if=col < 2)
    visit(3, both(dn2, col < 3), relayed=True)
    visit(6, dn1, relayed=True)
    visit(2, both(dn2, col < 2), relayed=True)
    visit(1, both(dn2, col < 1), relayed=True)

    per = g // 2
    o_copy = [pltpu.make_async_remote_copy(src_ref=o_send.at[oh, part], dst_ref=o_all.at[part], send_sem=os_sem.at[part], recv_sem=or_sem.at[part],
                                           device_id=dev(c, oh), device_id_type=MESH) for part in range(2)]
    with jax.named_scope("finish"):
        for part in range(2):
            for n in range(per):
                o = (acc[part * per + n] / l_s[part * per + n]).T.astype(BF16)
                for t in range(2):
                    o_send[t, part, :, n * hd:(n + 1) * hd] = o[t * tok:(t + 1) * tok]
            o_copy[part].start()
    with jax.named_scope("wowait"):
        ld_o.wait()
    n_y = 4
    cols = dm // n_y

    def project(o, core, part, cs):
        w = pl.multiple_of((2 * core + part) * per * hd, per * hd)
        return jnp.dot(o, wob[pl.ds(w, per * hd), cs], preferred_element_type=F32)

    spans = [slice(i * cols, (i + 1) * cols) for i in range(n_y)]
    with jax.named_scope("wo_own"):
        for cs in spans:
            y_v[:, cs] = project(o_send[h, 0], h, 0, cs) + project(o_send[h, 1], h, 1, cs)
    with jax.named_scope("owait"):
        o_copy[0].wait_recv()
    with jax.named_scope("wo_oth"):
        for cs in spans:
            y_v[:, cs] += project(o_all[0], oh, 0, cs)
    with jax.named_scope("owait2"):
        o_copy[1].wait_recv()
    with jax.named_scope("wo_oth2"):
        for cs in spans:
            y_ref[:, cs] = (y_v[:, cs] + project(o_all[1], oh, 1, cs)).astype(BF16)
    with jax.named_scope("sendwait"):
        x_copy.wait_send()
        for cp in p_copy:
            cp.wait_send()
        for cp in o_copy:
            cp.wait_send()
        each_direct(lambda cp: cp.wait_send(), 0, direct + later)

        for part in range(2):
            each_relay(lambda cp: cp.wait_send(), relays, part)


def solution(mesh):
    n_outer, n_inner = mesh.shape['cpo'], mesh.shape['cpi']

    def local_fn(hidden, w_q, w_k, w_v, w_o):
        tok, dm = hidden.shape
        hq, hd = w_q.shape[1], w_q.shape[2]
        g = hq // 2
        nb = WINDOW // (2 * tok) + 1
        loc, bas = rope_tables(2 * tok, n_outer * n_inner // 2, hd)
        dims = (n_outer, n_inner, tok, dm, g, hd, nb)
        scratch = [
            pltpu.VMEM((2, tok, dm), BF16), pltpu.VMEM((dm, g, hd), BF16), pltpu.VMEM((2 * dm, hd), BF16), pltpu.VMEM((2 * dm, hd), BF16),
            pltpu.VMEM((dm * g, hd), F32), pltpu.VMEM((hq * hd, dm), BF16),
            pltpu.VMEM(loc.shape, F32), pltpu.VMEM(bas.shape, F32),
            pltpu.VMEM((2, 2, tok, hd), BF16), pltpu.VMEM((nb, 2, 2, tok, hd), BF16),
            pltpu.VMEM((g, hd, 2 * tok), BF16), pltpu.VMEM((2, hd // 2, 2 * tok), F32),
            pltpu.VMEM((g, 1, 2 * tok), F32), pltpu.VMEM((g, 1, 2 * tok), F32), pltpu.VMEM((g, hd, 2 * tok), F32),
            pltpu.VMEM((2, tok, g * hd // 2), BF16), pltpu.VMEM((2, 2, tok, g * hd // 2), BF16), pltpu.VMEM((tok, dm), F32),
            pltpu.SemaphoreType.DMA((8,)), pltpu.SemaphoreType.DMA((4,)), pltpu.SemaphoreType.DMA, pltpu.SemaphoreType.DMA,
            pltpu.SemaphoreType.DMA((2,)), pltpu.SemaphoreType.DMA((2,)), pltpu.SemaphoreType.DMA((nb, 2, 2)), pltpu.SemaphoreType.DMA((nb, 2, 2)),
            pltpu.SemaphoreType.DMA((nb, 2)), pltpu.SemaphoreType.DMA((nb, 2)), pltpu.SemaphoreType.DMA((2,)), pltpu.SemaphoreType.DMA((2,)),
        ]
        return pl.pallas_call(
            functools.partial(kernel, dims),
            out_shape=pltpu.VMEM((tok, dm), BF16),
            in_specs=[pl.BlockSpec(memory_space=pl.ANY)] * 7,
            out_specs=pl.BlockSpec(memory_space=pltpu.VMEM),
            scratch_shapes=scratch,
            compiler_params=pltpu.CompilerParams(collective_id=0, has_side_effects=True, vmem_limit_bytes=56 * 1024 * 1024),
        )(hidden, w_q, w_k.reshape(2 * dm, hd), w_v.reshape(2 * dm, hd), w_o.reshape(hq * hd, dm), jnp.asarray(loc), jnp.asarray(bas))

    return jax.shard_map(local_fn, mesh=mesh,
                         in_specs=(P(('dp', 'cpo', 'cpi'), None), P(), P(), P(), P()),
                         out_specs=P(('dp', 'cpo', 'cpi'), None), check_vma=False)
```

```python
import functools
import math

import jax
import jax.numpy as jnp
import numpy as np
from jax import lax
from jax.experimental import pallas as pl
from jax.experimental.pallas import tpu as pltpu
from jax.sharding import PartitionSpec as P

WINDOW = 2048
ROPE_BASE = 10000.0
MESH = pl.DeviceIdType.MESH
F32, BF16 = jnp.float32, jnp.bfloat16


def rope_tables(tok_chip, n_chips, head_dim):
    half = head_dim // 2
    freq = ROPE_BASE ** (-np.arange(half, dtype=np.float64) * 2.0 / head_dim)
    local = np.arange(tok_chip, dtype=np.float64)[:, None] * freq
    base = (np.arange(n_chips, dtype=np.float64) * tok_chip)[:, None] * freq
    dup = lambda a: np.concatenate([a, a], axis=-1)
    loc = np.stack([dup(np.cos(local)), dup(np.sin(local))]).astype(np.float32)
    bas = np.stack([dup(np.cos(base)), dup(np.sin(base))]).astype(np.float32)
    return loc, bas


def kernel(dims, x_hbm, wq_hbm, wk_hbm, wv_hbm, wo_hbm, loc_hbm, bas_hbm, y_ref,
           x2, wqr, wkr, wvr, big, wob, loc, bas, own, kv, q_t, cs_t, m_s, l_s, acc, o_all, o_send, y_v,
           ld_sem, wq_sem, xs_sem, xr_sem, ps_sem, pr_sem, ks_sem, kr_sem, rs_sem, rr_sem, os_sem, or_sem):
    n_outer, n_inner, tok, dm, g, hd, nb = dims
    n_row = n_inner // 2
    n_chips = n_outer * n_inner // 2
    rank = lax.axis_index("cpo") * n_inner + lax.axis_index("cpi")
    c = lax.div(rank, 2)
    h = lax.rem(rank, 2)
    oh = 1 - h

    def dev(chip, core):
        r = chip * 2 + core
        return {"cpo": lax.div(r, n_inner), "cpi": lax.rem(r, n_inner)}

    def load(src, dst, sem):
        cp = pltpu.make_async_copy(src, dst, sem)
        cp.start()
        return cp

    row, col = lax.div(c, n_row), lax.rem(c, n_row)
    n_rows = n_chips // n_row
    last = nb - 1


    barrier = pltpu.get_barrier_semaphore()

    def greet(chip, core):
        pl.semaphore_signal(barrier, inc=1, device_id=dev(chip, core), device_id_type=MESH)

    right = row * n_row + lax.rem(col + 1, n_row)
    left = row * n_row + lax.rem(col + n_row - 1, n_row)
    one = lambda cond: jnp.where(cond, 1, 0)
    both = jnp.logical_and
    up1, up2, dn1, dn2 = row + 1 < n_rows, row + 2 < n_rows, row >= 1, row >= 2

    odd = lax.rem(row, 2) == 1
    direct = [(up1, 4, c + 4), (col < 3, 1, c + 1), (col < 1, 3, c + 3), (col < 2, 2, c + 2), (both(up2, odd), 8, c + 8)]
    edge = lax.rem(row, 4) == 0
    later = [(both(up2, edge), 8, c + 8)]
    origin = [(dn1, c - 4), (col >= 1, c - 1), (both(dn2, jnp.logical_not(edge)), c - 8), (col >= 3, c - 3), (col >= 2, c - 2)]
    relay_row = [(both(dn1, both(up1, lax.rem(row, 4) == 3)), 4, 8, c + 4), (dn1, 4, 5, right), (dn1, 4, 7, left)]
    relay_far = [(both(dn2, col >= 1), 8, 3, left), (both(dn2, col == 3), 8, 1, right), (both(dn2, col >= 2), 8, 2, c - 2)]
    relay_5 = [(both(dn1, col < 2), 5, 6, right)]
    relay_7 = [(both(dn1, col < 2), 7, 6, left)]

    def when_all(cond, act):
        pl.when(cond)(act)

    greet(c, oh)
    for cond, chip in origin:
        when_all(cond, lambda chip=chip: [greet(chip, hh) for hh in range(2)] and None)
    when_all(dn1, lambda: [greet(chip, h) for chip in (left, right)] and None)
    when_all(both(dn2, col < 2), lambda: greet(c + 2, h))
    n_sent = 1 + 2 * one(dn1) + one(both(dn2, col >= 2))
    for cond, _, _ in direct + later:
        n_sent = n_sent + 2 * one(cond)

    ld_x = load(x_hbm, x2.at[h], ld_sem.at[0])
    ld_k = [load(wk_hbm.at[pl.ds(i * dm, dm)], wkr.at[pl.ds(i * dm, dm)], ld_sem.at[1 + i]) for i in range(2)]
    ld_v = [load(wv_hbm.at[pl.ds(i * dm, dm)], wvr.at[pl.ds(i * dm, dm)], ld_sem.at[6 + i]) for i in range(2)]
    ld_l = load(loc_hbm, loc, ld_sem.at[3])
    ld_b = load(bas_hbm, bas, ld_sem.at[4])
    def unpack(src, dst_row, rows):
        step = 1024

        def body(t, _):
            r = pl.multiple_of(t * step, step)
            big[pl.ds(pl.multiple_of(dst_row + r, step), step), :] = src[pl.ds(r, step), :].astype(F32)
            return 0

        lax.fori_loop(0, rows // step, body, 0)

    def columns(first, start, stride):
        return [big[pl.ds(first + s, dm, stride=stride), :].astype(BF16) for s in range(start, start + 2)]

    with jax.named_scope("relay_kv"):
        for ld in ld_k:
            ld.wait()
        unpack(wkr, 0, 2 * dm)
    ld_x.wait()
    with jax.named_scope("kvproj"):
        kp = jnp.dot(x2[h], jnp.concatenate(columns(0, 0, 2), axis=1), preferred_element_type=F32)
        for ld in ld_v:
            ld.wait()
        unpack(wvr, 2 * dm, 2 * dm)
        n_wq = wq_sem.shape[0]
        rows_wq = dm // n_wq
        head0 = pl.multiple_of(h * g, g)
        ld_q = [load(wq_hbm.at[pl.ds(i * rows_wq, rows_wq), pl.ds(head0, g), :], wqr.at[pl.ds(i * rows_wq, rows_wq)], wq_sem.at[i])
                for i in range(n_wq)]
        vp = jnp.dot(x2[h], jnp.concatenate(columns(2 * dm, 0, 2), axis=1), preferred_element_type=F32)
    ld_l.wait()
    ld_b.wait()
    t0 = pl.multiple_of(h * tok, tok)
    cb, sb = bas[0, pl.ds(c, 1), :], bas[1, pl.ds(c, 1), :]
    cl, sl = loc[0, pl.ds(t0, tok), :], loc[1, pl.ds(t0, tok), :]
    cos_k = cl * cb - sl * sb
    sin_k = sl * cb + cl * sb
    lane = lax.broadcasted_iota(jnp.int32, (tok, hd), 1)
    sin_k = jnp.where(lane < hd // 2, -sin_k, sin_k)
    for hh in range(2):
        k = kp[:, hh * hd:(hh + 1) * hd]
        k = (k * cos_k + pltpu.roll(k, hd // 2, 1) * sin_k).astype(BF16)
        v = vp[:, hh * hd:(hh + 1) * hd]
        own[hh, 0] = k
        own[hh, 1] = v.T.astype(BF16)
    kv[0, 0, h] = own[h, 0]
    kv[0, 1, h] = own[h, 1]

    with jax.named_scope("barrier"):
        pl.semaphore_wait(barrier, n_sent)
    x_copy = pltpu.make_async_remote_copy(src_ref=x2.at[h], dst_ref=x2.at[h], send_sem=xs_sem, recv_sem=xr_sem,
                                          device_id=dev(c, oh), device_id_type=MESH)

    p_copy = [pltpu.make_async_remote_copy(src_ref=own.at[oh, part], dst_ref=kv.at[0, part, h], send_sem=ps_sem.at[part], recv_sem=pr_sem.at[part],
                                           device_id=dev(c, oh), device_id_type=MESH) for part in range(2)]

    def each_direct(act, first, group):
        for i, (cond, slot, chip) in enumerate(group, first):
            @pl.when(cond)
            def _():
                for part in range(2):
                    for hh in range(2):
                        act(pltpu.make_async_remote_copy(src_ref=own.at[hh, part], dst_ref=kv.at[slot, part, h], send_sem=ks_sem.at[i, part, hh],
                                                         recv_sem=kr_sem.at[slot, part, h], device_id=dev(chip, hh), device_id_type=MESH))

    relays = relay_row + relay_far + relay_5 + relay_7

    def each_relay(act, group, part):
        for item in group:
            cond, src, dst, chip = item
            i = [r is item for r in relays].index(True)

            @pl.when(cond)
            def _():
                act(pltpu.make_async_remote_copy(src_ref=kv.at[src, part], dst_ref=kv.at[dst, part], send_sem=rs_sem.at[i, part],
                                                 recv_sem=rr_sem.at[dst, part], device_id=dev(chip, h), device_id_type=MESH))

    each_direct(lambda cp: cp.start(), 0, direct[:1])
    for cp in p_copy:
        cp.start()
    each_direct(lambda cp: cp.start(), 1, direct[1:])
    x_copy.start()

    ld_o = load(wo_hbm, wob, ld_sem.at[5])

    with jax.named_scope("relay_q"):
        dch = 128
        for i in range(n_wq):
            ld_q[i].wait()

            def unpack_q(t, _):
                d0 = pl.multiple_of(i * rows_wq + t * dch, dch)
                big[pl.ds(pl.multiple_of(d0 * g, dch * g), dch * g), :] = wqr[pl.ds(d0, dch)].astype(F32).reshape(dch * g, hd)
                return 0

            lax.fori_loop(0, rows_wq // dch, unpack_q, 0)
    each_direct(lambda cp: cp.start(), len(direct), later)
    half = hd // 2
    cl, sl = loc[0], loc[1]
    cs_t[0] = (cl * cb - sl * sb).T[:half]
    cs_t[1] = (sl * cb + cl * sb).T[:half]
    with jax.named_scope("xwait"):
        x_copy.wait_recv()
    xall = x2[...].reshape(2 * tok, dm)

    def landed(slot, relayed, group=(), parts=(0, 1)):
        for part in parts:
            with jax.named_scope(f"w{slot}{'kv'[part]}{'r' * relayed}"):
                if relayed:
                    pltpu.make_async_copy(kv.at[0, part], kv.at[slot, part], rr_sem.at[slot, part]).wait()
                else:
                    for s in range(2):
                        pltpu.make_async_copy(own.at[0, part], kv.at[slot, part, s], kr_sem.at[slot, part, s]).wait()
            each_relay(lambda cp: cp.start(), group, part)

    third = both(dn1, lax.rem(row, 4) == 3)
    early = lambda part: pl.when(third)(lambda: landed(4, False, relay_row, (part,)))

    def proj_q(n):
        return jnp.dot(xall, jnp.concatenate(columns(0, 2 * n, g), axis=1), preferred_element_type=F32)

    with jax.named_scope("qproj"):
        for n in range(g // 2):
            if n == g // 2 - 1:
                early(0)
            qp = proj_q(n)
            for s in range(2):
                qt = qp[:, s * hd:(s + 1) * hd].T
                lo, hi = qt[:half], qt[half:]
                q_t[2 * n + s, :half] = (lo * cs_t[0] - hi * cs_t[1]).astype(BF16)
                q_t[2 * n + s, half:] = (hi * cs_t[0] + lo * cs_t[1]).astype(BF16)
    scale = hd ** -0.5 * math.log2(math.e)
    ki = lax.broadcasted_iota(jnp.int32, (2 * tok, 2 * tok), 0)
    qi = lax.broadcasted_iota(jnp.int32, (2 * tok, 2 * tok), 1)

    def attend(slot):
        kb = kv[slot, 0].reshape(2 * tok, hd)
        vb = jnp.concatenate([kv[slot, 1, 0], kv[slot, 1, 1]], axis=1)

        def weigh(n, s):
            if slot == 0:
                s = jnp.where(ki <= qi, s, -jnp.inf)
            if slot == last:
                s = jnp.where(ki > qi, s, -jnp.inf)
            top = jnp.max(s, axis=0, keepdims=True) * scale
            m_new = top if slot == 0 else jnp.maximum(m_s[n], top)
            p = jnp.exp2(s * scale - m_new)
            tot = jnp.sum(p, axis=0, keepdims=True)
            alpha = None
            if slot == 0:
                l_s[n] = tot
            else:
                alpha = jnp.exp2(m_s[n] - m_new)
                l_s[n] = l_s[n] * alpha + tot
            m_s[n] = m_new
            return p.astype(BF16), alpha

        def gather(n, p, alpha):
            r = jnp.dot(vb, p, preferred_element_type=F32)
            acc[n] = r if alpha is None else acc[n] * alpha + r

        scores, held = [], []
        for n in range(g):
            while len(scores) < min(n + 5, g):
                scores.append(jnp.dot(kb, q_t[len(scores)], preferred_element_type=F32))
            held.append((n, *weigh(n, scores[n])))
            if len(held) > 3:
                gather(*held.pop(0))
        for item in held:
            gather(*item)

    def visit(slot, here, relayed=False, got_if=None, group=()):
        @pl.when(here)
        def _():
            if got_if is None:
                landed(slot, relayed, group)
            elif got_if is not True:
                pl.when(jnp.logical_not(got_if))(lambda: landed(slot, relayed, group))
            with jax.named_scope(f"att{slot}"):
                attend(slot)

    pl.when(both(dn1, lax.rem(row, 4) % 3 > 0))(lambda: landed(4, False, relay_row, (0,)))
    early(1)
    with jax.named_scope("pwait"):
        for cp in p_copy:
            cp.wait_recv()
    with jax.named_scope("att0"):
        attend(0)
    pl.when(both(dn1, edge))(lambda: landed(4, False, relay_row, (0,)))
    pl.when(both(dn1, jnp.logical_not(third)))(lambda: landed(4, False, relay_row, (1,)))
    visit(4, dn1, got_if=True)
    visit(1, col >= 1)
    slow = both(edge, col < 2)

    @pl.when(both(dn2, jnp.logical_not(edge)))
    def _():
        landed(8, False, relay_far)

    @pl.when(both(dn2, edge))
    def _():
        landed(8, True, relay_far, (0,))

        @pl.when(col < 2)
        def _():
            landed(5, True, relay_5, (0,))
            landed(7, True, relay_7, (0,))
        landed(8, True, relay_far, (1,))

    visit(8, dn2, got_if=True)

    @pl.when(both(dn1, col < 2))
    def _():
        @pl.when(jnp.logical_not(slow))
        def _():
            landed(5, True, relay_5, (0,))
            landed(7, True, relay_7, (0,))
        landed(5, True, relay_5, (1,))
        landed(7, True, relay_7, (1,))

    visit(2, col >= 2)
    visit(3, col >= 3)
    visit(5, dn1, relayed=True, got_if=col < 2)
    visit(7, dn1, relayed=True, got_if=col < 2)
    visit(3, both(dn2, col < 3), relayed=True)
    visit(6, dn1, relayed=True)
    visit(2, both(dn2, col < 2), relayed=True)
    visit(1, both(dn2, col < 1), relayed=True)

    per = g // 2
    o_copy = [pltpu.make_async_remote_copy(src_ref=o_send.at[oh, part], dst_ref=o_all.at[part], send_sem=os_sem.at[part], recv_sem=or_sem.at[part],
                                           device_id=dev(c, oh), device_id_type=MESH) for part in range(2)]
    with jax.named_scope("finish"):
        for part in range(2):
            for n in range(per):
                o = (acc[part * per + n] / l_s[part * per + n]).T.astype(BF16)
                for t in range(2):
                    o_send[t, part, :, n * hd:(n + 1) * hd] = o[t * tok:(t + 1) * tok]
            o_copy[part].start()
    with jax.named_scope("wowait"):
        ld_o.wait()
    n_y = 4
    cols = dm // n_y

    def project(o, core, part, cs):
        w = pl.multiple_of((2 * core + part) * per * hd, per * hd)
        return jnp.dot(o, wob[pl.ds(w, per * hd), cs], preferred_element_type=F32)

    spans = [slice(i * cols, (i + 1) * cols) for i in range(n_y)]
    with jax.named_scope("wo_own"):
        for cs in spans:
            y_v[:, cs] = project(o_send[h, 0], h, 0, cs) + project(o_send[h, 1], h, 1, cs)
    with jax.named_scope("owait"):
        o_copy[0].wait_recv()
    with jax.named_scope("wo_oth"):
        for cs in spans:
            y_v[:, cs] += project(o_all[0], oh, 0, cs)
    with jax.named_scope("owait2"):
        o_copy[1].wait_recv()
    with jax.named_scope("wo_oth2"):
        for cs in spans:
            y_ref[:, cs] = (y_v[:, cs] + project(o_all[1], oh, 1, cs)).astype(BF16)
    with jax.named_scope("sendwait"):
        x_copy.wait_send()
        for cp in p_copy:
            cp.wait_send()
        for cp in o_copy:
            cp.wait_send()
        each_direct(lambda cp: cp.wait_send(), 0, direct + later)

        for part in range(2):
            each_relay(lambda cp: cp.wait_send(), relays, part)


def solution(mesh):
    n_outer, n_inner = mesh.shape['cpo'], mesh.shape['cpi']

    def local_fn(hidden, w_q, w_k, w_v, w_o):
        tok, dm = hidden.shape
        hq, hd = w_q.shape[1], w_q.shape[2]
        g = hq // 2
        nb = WINDOW // (2 * tok) + 1
        loc, bas = rope_tables(2 * tok, n_outer * n_inner // 2, hd)
        dims = (n_outer, n_inner, tok, dm, g, hd, nb)
        scratch = [
            pltpu.VMEM((2, tok, dm), BF16), pltpu.VMEM((dm, g, hd), BF16), pltpu.VMEM((2 * dm, hd), BF16), pltpu.VMEM((2 * dm, hd), BF16),
            pltpu.VMEM((dm * g, hd), F32), pltpu.VMEM((hq * hd, dm), BF16),
            pltpu.VMEM(loc.shape, F32), pltpu.VMEM(bas.shape, F32),
            pltpu.VMEM((2, 2, tok, hd), BF16), pltpu.VMEM((nb, 2, 2, tok, hd), BF16),
            pltpu.VMEM((g, hd, 2 * tok), BF16), pltpu.VMEM((2, hd // 2, 2 * tok), F32),
            pltpu.VMEM((g, 1, 2 * tok), F32), pltpu.VMEM((g, 1, 2 * tok), F32), pltpu.VMEM((g, hd, 2 * tok), F32),
            pltpu.VMEM((2, tok, g * hd // 2), BF16), pltpu.VMEM((2, 2, tok, g * hd // 2), BF16), pltpu.VMEM((tok, dm), F32),
            pltpu.SemaphoreType.DMA((8,)), pltpu.SemaphoreType.DMA((4,)), pltpu.SemaphoreType.DMA, pltpu.SemaphoreType.DMA,
            pltpu.SemaphoreType.DMA((2,)), pltpu.SemaphoreType.DMA((2,)), pltpu.SemaphoreType.DMA((nb, 2, 2)), pltpu.SemaphoreType.DMA((nb, 2, 2)),
            pltpu.SemaphoreType.DMA((nb, 2)), pltpu.SemaphoreType.DMA((nb, 2)), pltpu.SemaphoreType.DMA((2,)), pltpu.SemaphoreType.DMA((2,)),
        ]
        return pl.pallas_call(
            functools.partial(kernel, dims),
            out_shape=pltpu.VMEM((tok, dm), BF16),
            in_specs=[pl.BlockSpec(memory_space=pl.ANY)] * 7,
            out_specs=pl.BlockSpec(memory_space=pltpu.VMEM),
            scratch_shapes=scratch,
            compiler_params=pltpu.CompilerParams(collective_id=0, has_side_effects=True, vmem_limit_bytes=56 * 1024 * 1024),
        )(hidden, w_q, w_k.reshape(2 * dm, hd), w_v.reshape(2 * dm, hd), w_o.reshape(hq * hd, dm), jnp.asarray(loc), jnp.asarray(bas))

    return jax.shard_map(local_fn, mesh=mesh,
                         in_specs=(P(('dp', 'cpo', 'cpi'), None), P(), P(), P(), P()),
                         out_specs=P(('dp', 'cpo', 'cpi'), None), check_vma=False)
```
